32 devices in a mesh: dp: 4 (over y, z), tp: 8 (over x, core).
Axes of the slice: x: 4, y: 2, z: 2, core: 2. Of those that a mesh axis runs over, the one named last changes fastest.
The devices are a block of a 4x4x8 slice.
Arguments:
- hidden: bfloat16 [32, 2048, 1024], P('dp', 'tp'), parts along dimension 0
- attn_gain: float32 [1024], replicated
- attn_bias: float32 [1024], replicated
- mlp_gain: float32 [1024], replicated
- mlp_bias: float32 [1024], replicated
- w_qkv: bfloat16 [1024, 16, 192], P(None, 'tp')
- w_out: bfloat16 [1024, 1024], P('tp')
- w_up: bfloat16 [1024, 4096], P(None, 'tp')
- w_down: bfloat16 [4096, 1024], P('tp')
- positions: int32 [2048], replicated
Outputs:
- output: bfloat16 [32, 2048, 1024], P('dp', 'tp'), parts along dimension 0
There are 4 independent parts. The reference program is written for one: setup_inputs(seed, part) draws one part's arguments, and reference() takes and returns one part's arrays. A program takes and returns all parts, laid end to end along the dimension named above; an argument that names none is the same for every part.
All inputs are finite; a program needn't handle non-finite values.
Results may differ from the reference program's by a relative error of at most 0.00413463.
Values are sent between devices in bfloat16 or wider.
A program may use at most 768 MiB of HBM per device.

```python
import jax
import jax.numpy as jnp
from jax import lax

D = 1024
HEADS = 16
KV_HEADS = 16
HEAD = 64
FF = 4096
BATCH = 8
SEQ_LEN = 2048
QUERY_BLOCK = 64
HALF_HEAD = 32

GROUP_SIZE = HEADS // KV_HEADS
QKV_COLS = (GROUP_SIZE + 2) * HEAD


def setup_inputs(seed: int = 0, part: int = 0) -> dict:
    root_key = jax.random.key(seed)
    sub_keys = jax.random.split(root_key, 10)
    part_key = jax.random.fold_in(sub_keys[0], part)
    hidden = jax.random.normal(part_key, (BATCH, SEQ_LEN, D), jnp.float32).astype(jnp.bfloat16)
    attn_gain = 1.0 + 0.4 * jax.random.normal(sub_keys[1], (D,), jnp.float32)
    attn_bias = 0.4 * jax.random.normal(sub_keys[2], (D,), jnp.float32)
    mlp_gain = 1.0 + 0.4 * jax.random.normal(sub_keys[3], (D,), jnp.float32)
    mlp_bias = 0.4 * jax.random.normal(sub_keys[4], (D,), jnp.float32)
    w_qkv = (1.2 * D ** -0.5 * jax.random.normal(sub_keys[5], (D, KV_HEADS, QKV_COLS), jnp.float32)).astype(jnp.bfloat16)
    w_out = (2.0 * (HEADS * HEAD) ** -0.5 * jax.random.normal(sub_keys[6], (HEADS * HEAD, D), jnp.float32)).astype(jnp.bfloat16)
    w_up = (D ** -0.5 * jax.random.normal(sub_keys[7], (D, FF), jnp.float32)).astype(jnp.bfloat16)
    w_down = (FF ** -0.5 * jax.random.normal(sub_keys[8], (FF, D), jnp.float32)).astype(jnp.bfloat16)
    pos_gaps = jax.random.randint(sub_keys[9], (SEQ_LEN,), 1, 4, jnp.int32)
    positions = (jnp.cumsum(pos_gaps) - pos_gaps[0]).astype(jnp.int32)
    return {'hidden': hidden, 'attn_gain': attn_gain, 'attn_bias': attn_bias, 'mlp_gain': mlp_gain, 'mlp_bias': mlp_bias, 'w_qkv': w_qkv, 'w_out': w_out, 'w_up': w_up, 'w_down': w_down, 'positions': positions}


def layer_norm(tok_rows, norm_gain, norm_bias):
    rows32 = tok_rows.astype(jnp.float32)
    row_mean = jnp.mean(rows32, axis=-1, keepdims=True)
    centered = rows32 - row_mean
    row_var = jnp.mean(centered * centered, axis=-1, keepdims=True)
    return (centered * lax.rsqrt(row_var + 1e-5) * norm_gain + norm_bias).astype(jnp.bfloat16)


def apply_rotary(head_vals, cos_tab, sin_tab):
    vals32 = head_vals.astype(jnp.float32)
    rotated = jnp.concatenate([-vals32[..., HALF_HEAD:], vals32[..., :HALF_HEAD]], axis=-1)
    return (vals32 * cos_tab + rotated * sin_tab).astype(jnp.bfloat16)


def attend_sequence(query_rot, key_rot, value_seq):
    key32 = key_rot.astype(jnp.float32)
    value32 = value_seq.astype(jnp.float32)
    key_idx = jnp.arange(SEQ_LEN)

    def one_block(block_idx):
        row_start = block_idx * QUERY_BLOCK
        query_blk = lax.dynamic_slice_in_dim(query_rot, row_start, QUERY_BLOCK, axis=0).astype(jnp.float32)
        scores = jnp.einsum('qkgh,skh->kgqs', query_blk, key32) * HEAD ** -0.5
        query_idx = row_start + jnp.arange(QUERY_BLOCK)
        allowed = key_idx[None, :] <= query_idx[:, None]
        scores = jnp.where(allowed, scores, -1e30)
        exp_scores = jnp.exp(scores - jnp.max(scores, axis=-1, keepdims=True))
        attn_probs = (exp_scores / jnp.sum(exp_scores, axis=-1, keepdims=True)).astype(jnp.bfloat16)
        context = jnp.einsum('kgqs,skh->qkgh', attn_probs.astype(jnp.float32), value32)
        return context.astype(jnp.bfloat16)

    ctx_blocks = lax.map(one_block, jnp.arange(SEQ_LEN // QUERY_BLOCK))
    return ctx_blocks.reshape(SEQ_LEN, HEADS * HEAD)


def reference(hidden, attn_gain, attn_bias, mlp_gain, mlp_bias, w_qkv, w_out, w_up, w_down, positions):
    inv_freq = 10000.0 ** (-2.0 * jnp.arange(HALF_HEAD, dtype=jnp.float32) / HEAD)
    angles = positions.astype(jnp.float32)[:, None] * inv_freq[None, :]
    angles = jnp.concatenate([angles, angles], axis=-1)
    cos_tab = jnp.cos(angles)
    sin_tab = jnp.sin(angles)
    w_qkv_flat = w_qkv.reshape(D, KV_HEADS * QKV_COLS)

    def one_sequence(seq_rows):
        normed_attn = layer_norm(seq_rows, attn_gain, attn_bias)
        normed_mlp = layer_norm(seq_rows, mlp_gain, mlp_bias)
        qkv_rows = jnp.dot(normed_attn, w_qkv_flat, preferred_element_type=jnp.float32).astype(jnp.bfloat16)
        qkv_rows = qkv_rows.reshape(SEQ_LEN, KV_HEADS, GROUP_SIZE + 2, HEAD)
        query_rot = apply_rotary(qkv_rows[:, :, :GROUP_SIZE, :], cos_tab[:, None, None, :], sin_tab[:, None, None, :])
        key_rot = apply_rotary(qkv_rows[:, :, GROUP_SIZE, :], cos_tab[:, None, :], sin_tab[:, None, :])
        value_seq = qkv_rows[:, :, GROUP_SIZE + 1, :]
        context = attend_sequence(query_rot, key_rot, value_seq)
        attn_part = jnp.dot(context, w_out, preferred_element_type=jnp.float32)
        up_pre = jnp.dot(normed_mlp, w_up, preferred_element_type=jnp.float32)
        up_act = jax.nn.gelu(up_pre, approximate=False).astype(jnp.bfloat16)
        mlp_part = jnp.dot(up_act, w_down, preferred_element_type=jnp.float32)
        return (seq_rows.astype(jnp.float32) + attn_part + mlp_part).astype(jnp.bfloat16)

    return lax.map(one_sequence, hidden)
```

```python
import functools

import jax
import jax.numpy as jnp
from jax import lax
from jax.experimental import pallas as pl
from jax.experimental.pallas import tpu as pltpu
from jax.sharding import PartitionSpec as P

BF16 = jnp.bfloat16
F32 = jnp.float32
VMEM_LIMIT = 60 * 1024 * 1024


def norm_rows(rows, gain, bias):
    rows32 = rows.astype(F32)
    mean = jnp.mean(rows32, axis=-1, keepdims=True)
    centered = rows32 - mean
    var = jnp.mean(centered * centered, axis=-1, keepdims=True)
    return (centered * lax.rsqrt(var + 1e-5) * gain + bias).astype(BF16)


def swap_halves(vals, lane_mod, half):
    width = vals.shape[-1]
    return jnp.where(lane_mod < half, pltpu.roll(vals, width - half, 1), pltpu.roll(vals, half, 1))


def qkv_kernel(head_dim, x_ref, w_ref, cos_ref, sin_ref, gain_ref, bias_ref, q_ref, k_ref, v_ref):
    blocks, rows, width = x_ref.shape
    normed = norm_rows(x_ref[...].reshape(blocks * rows, width), gain_ref[...], bias_ref[...])
    pair = q_ref.shape[2]
    cos_tab, sin_tab = cos_ref[...], sin_ref[...]
    lane_mod = lax.broadcasted_iota(jnp.int32, cos_tab.shape, 1) % head_dim
    scale = head_dim ** -0.5

    def rotate(vals):
        vals = vals.astype(BF16).astype(F32)
        return (vals * cos_tab + swap_halves(vals, lane_mod, head_dim // 2) * sin_tab).astype(BF16)

    for p in range(w_ref.shape[0]):
        qkv = jnp.dot(normed, w_ref[p], preferred_element_type=F32)
        q_ref[p] = (rotate(qkv[:, :pair]).astype(F32) * scale).astype(BF16)
        k_ref[p] = rotate(qkv[:, pair:2 * pair]).astype(F32).T.astype(BF16)
        v_ref[p] = qkv[:, 2 * pair:].astype(BF16)


def attn_kernel(head_dim, q_ref, k_ref, v_ref, o_ref, s_ref):
    block = q_ref.shape[1]
    pair = q_ref.shape[2]
    heads = pair // head_dim
    num_blocks = k_ref.shape[2] // block

    def one_block(i):
        q = q_ref[0]
        lane = lax.broadcasted_iota(jnp.int32, q.shape, 1)
        zero = jnp.zeros_like(q)
        q_all = jnp.concatenate([jnp.where(lane // head_dim == h, q, zero) for h in range(heads)], axis=0)
        m = None
        for c in range(i + 1):
            s = jnp.dot(q_all, k_ref[0, :, c * block:(c + 1) * block], preferred_element_type=F32)
            if c == i:
                row = lax.broadcasted_iota(jnp.int32, s.shape, 0) % block
                col = lax.broadcasted_iota(jnp.int32, s.shape, 1)
                s = jnp.where(col <= row, s, -1e30)
            s_ref[:, c * block:(c + 1) * block] = s
            part = functools.reduce(jnp.maximum, [s[:, t:t + 128] for t in range(0, block, 128)])
            m = part if m is None else jnp.maximum(m, part)
        m = jnp.max(m, axis=1, keepdims=True)
        total, acc = None, None
        for c in range(i + 1):
            e = jnp.exp(s_ref[:, c * block:(c + 1) * block] - m)
            part = functools.reduce(jnp.add, [e[:, t:t + 128] for t in range(0, block, 128)])
            total = part if total is None else total + part
            pv = jnp.dot(e.astype(BF16), v_ref[0, c * block:(c + 1) * block, :], preferred_element_type=F32)
            acc = pv if acc is None else acc + pv
        out = acc / jnp.sum(total, axis=1, keepdims=True)
        lane_out = lax.broadcasted_iota(jnp.int32, (block, pair), 1)
        res = out[:block]
        for h in range(1, heads):
            res = jnp.where(lane_out // head_dim == h, out[h * block:(h + 1) * block], res)
        o_ref[...] = res.astype(BF16)

    for i in range(num_blocks):
        pl.when(pl.program_id(1) == i)(functools.partial(one_block, i))


def mlp_kernel(x_ref, gain_ref, bias_ref, up_ref, down_ref, o_ref, m_ref, acc_ref):
    f, t = pl.program_id(0), pl.program_id(1)
    rows = x_ref.shape[0]
    sl = pl.ds(pl.multiple_of(t * rows, rows), rows)

    @pl.when(f == 0)
    def _():
        m_ref[sl, :] = norm_rows(x_ref[...], gain_ref[...], bias_ref[...])

    half = rows // 2
    for h in range(2):
        part = pl.ds(pl.multiple_of(t * rows + h * half, half), half)
        pre = jnp.dot(m_ref[part, :], up_ref[0], preferred_element_type=F32)
        act = (0.5 * pre * (1.0 + lax.erf(pre * (0.5 ** 0.5)))).astype(BF16)
        down = jnp.dot(act, down_ref[0], preferred_element_type=F32)

        @pl.when(f == 0)
        def _(part=part, down=down):
            acc_ref[part, :] = down

        @pl.when(f > 0)
        def _(part=part, down=down):
            acc_ref[part, :] += down

    @pl.when(f == pl.num_programs(0) - 1)
    def _():
        o_ref[...] = acc_ref[sl, :]


def final_kernel(x_ref, ctx_ref, wo_ref, mlp_ref, y_ref):
    attn = jnp.dot(ctx_ref[...], wo_ref[...], preferred_element_type=F32)
    y_ref[...] = (x_ref[...].astype(F32) + attn + mlp_ref[...]).astype(BF16)


def params(sem):
    return pltpu.CompilerParams(dimension_semantics=sem, vmem_limit_bytes=VMEM_LIMIT)


def solution(mesh):
    tp = mesh.shape['tp']

    def local_layer(x, attn_gain, attn_bias, mlp_gain, mlp_bias, w_qkv, w_out, w_up, w_down, positions):
        batch, chunk, width = x.shape
        per_dev = batch // tp
        groups, slot_cols = w_qkv.shape[1:]
        ctx_cols = w_out.shape[0]
        head_dim = (slot_cols - ctx_cols // groups) // 2
        pair = groups * head_dim
        seq = chunk * tp
        ff = w_up.shape[1]
        tokens = batch * chunk
        half = head_dim // 2

        w_qkv = w_qkv.reshape(width, groups, 3, head_dim).swapaxes(1, 2).reshape(width, 3 * pair)
        wqkv_all = lax.all_gather(w_qkv, 'tp', axis=0, tiled=False)
        x_seq = lax.all_to_all(x, 'tp', split_axis=0, concat_axis=0, tiled=True)
        x_seq = x_seq.reshape(tp, chunk, width)

        inv_freq = 10000.0 ** (-2.0 * jnp.arange(half, dtype=F32) / head_dim)
        inv_freq = jnp.tile(inv_freq, 2 * groups)
        angles = positions.astype(F32)[:, None] * inv_freq[None, :]
        sign = jnp.where(jnp.arange(pair) % head_dim < half, -1.0, 1.0).astype(F32)
        cos_tab, sin_tab = jnp.cos(angles), jnp.sin(angles) * sign[None, :]

        gain2, bias2 = attn_gain.reshape(1, width), attn_bias.reshape(1, width)
        nb = 2
        q, k, v = pl.pallas_call(
            functools.partial(qkv_kernel, head_dim),
            grid=(tp // nb,),
            in_specs=[
                pl.BlockSpec((nb, chunk, width), lambda i: (i, 0, 0)),
                pl.BlockSpec((tp, width, 3 * pair), lambda i: (0, 0, 0)),
                pl.BlockSpec((nb * chunk, pair), lambda i: (i, 0)),
                pl.BlockSpec((nb * chunk, pair), lambda i: (i, 0)),
                pl.BlockSpec((1, width), lambda i: (0, 0)),
                pl.BlockSpec((1, width), lambda i: (0, 0)),
            ],
            out_specs=[
                pl.BlockSpec((tp, nb * chunk, pair), lambda i: (0, i, 0)),
                pl.BlockSpec((tp, pair, nb * chunk), lambda i: (0, 0, i)),
                pl.BlockSpec((tp, nb * chunk, pair), lambda i: (0, i, 0)),
            ],
            out_shape=[
                jax.ShapeDtypeStruct((tp, seq, pair), BF16),
                jax.ShapeDtypeStruct((tp, pair, seq), BF16),
                jax.ShapeDtypeStruct((tp, seq, pair), BF16),
            ],
            compiler_params=params(('arbitrary',)),
            cost_estimate=pl.CostEstimate(flops=2 * seq * width * 3 * pair * tp, bytes_accessed=2 * (seq * width * 4 + width * 3 * pair * tp), transcendentals=0),
            name='qkv',
        )(x_seq, wqkv_all, cos_tab, sin_tab, gain2, bias2)

        block = chunk
        ctx = pl.pallas_call(
            functools.partial(attn_kernel, head_dim),
            grid=(tp, seq // block),
            in_specs=[
                pl.BlockSpec((1, block, pair), lambda p, i: (p, i, 0)),
                pl.BlockSpec((1, pair, seq), lambda p, i: (p, 0, 0)),
                pl.BlockSpec((1, seq, pair), lambda p, i: (p, 0, 0)),
            ],
            out_specs=pl.BlockSpec((block, pair), lambda p, i: (i, p)),
            out_shape=jax.ShapeDtypeStruct((seq, tp * pair), BF16),
            scratch_shapes=[pltpu.VMEM((groups * block, seq), F32)],
            compiler_params=params(('arbitrary', 'arbitrary')),
            cost_estimate=pl.CostEstimate(flops=8 * seq * seq * pair * tp, bytes_accessed=2 * seq * width * 4, transcendentals=0),
            name='attn',
        )(q, k, v)

        w_up, w_down, w_out, _, _ = lax.optimization_barrier((w_up, w_down, w_out, wqkv_all, x_seq))
        up_all = lax.all_gather(w_up, 'tp', axis=0, tiled=False)
        down_all = lax.all_gather(w_down, 'tp', axis=0, tiled=False)
        wo_all = lax.all_gather(w_out, 'tp', axis=0, tiled=True)
        x_mlp, ctx = lax.optimization_barrier((x, ctx))
        ctx_own = lax.all_to_all(ctx.reshape(tp, chunk, width), 'tp', split_axis=0, concat_axis=0, tiled=True)
        x_rows = x_mlp.reshape(tokens, width)
        rows = 512
        nt = tokens // rows
        mlp = pl.pallas_call(
            mlp_kernel,
            grid=(tp, nt),
            in_specs=[
                pl.BlockSpec((rows, width), lambda f, t: (jnp.where(f == 0, t, nt - 1), 0)),
                pl.BlockSpec((1, width), lambda f, t: (0, 0)),
                pl.BlockSpec((1, width), lambda f, t: (0, 0)),
                pl.BlockSpec((1, width, ff), lambda f, t: (f, 0, 0)),
                pl.BlockSpec((1, ff, width), lambda f, t: (f, 0, 0)),
            ],
            out_specs=pl.BlockSpec((rows, width), lambda f, t: (jnp.where(f == tp - 1, t, 0), 0)),
            out_shape=jax.ShapeDtypeStruct((tokens, width), F32),
            scratch_shapes=[pltpu.VMEM((tokens, width), BF16), pltpu.VMEM((tokens, width), F32)],
            compiler_params=params(('arbitrary', 'arbitrary')),
            cost_estimate=pl.CostEstimate(flops=4 * tokens * width * ff * tp, bytes_accessed=4 * tokens * width * 2, transcendentals=0),
            name='mlp',
        )(x_rows, mlp_gain.reshape(1, width), mlp_bias.reshape(1, width), up_all, down_all)

        y = pl.pallas_call(
            final_kernel,
            grid=(nt,),
            in_specs=[
                pl.BlockSpec((rows, width), lambda t: (t, 0)),
                pl.BlockSpec((rows, width), lambda t: (t, 0)),
                pl.BlockSpec((width, width), lambda t: (0, 0)),
                pl.BlockSpec((rows, width), lambda t: (t, 0)),
            ],
            out_specs=pl.BlockSpec((rows, width), lambda t: (t, 0)),
            out_shape=jax.ShapeDtypeStruct((tokens, width), BF16),
            compiler_params=params(('arbitrary',)),
            cost_estimate=pl.CostEstimate(flops=2 * tokens * width * width, bytes_accessed=tokens * width * 10, transcendentals=0),
            name='final',
        )(x_rows, ctx_own.reshape(tokens, width), wo_all, mlp)
        return y.reshape(batch, chunk, width)

    return jax.shard_map(local_layer, mesh=mesh, in_specs=(P('dp', 'tp', None), P(), P(), P(), P(), P(None, 'tp', None), P('tp', None), P(None, 'tp'), P('tp', None), P()), out_specs=P('dp', 'tp', None), check_vma=False)
```

```python
import functools

import jax
import jax.numpy as jnp
from jax import lax
from jax.experimental import pallas as pl
from jax.experimental.pallas import tpu as pltpu
from jax.sharding import PartitionSpec as P

BF16 = jnp.bfloat16
F32 = jnp.float32
VMEM_LIMIT = 60 * 1024 * 1024


def norm_rows(rows, gain, bias):
    rows32 = rows.astype(F32)
    mean = jnp.mean(rows32, axis=-1, keepdims=True)
    centered = rows32 - mean
    var = jnp.mean(centered * centered, axis=-1, keepdims=True)
    return (centered * lax.rsqrt(var + 1e-5) * gain + bias).astype(BF16)


def swap_halves(vals, lane_mod, half):
    width = vals.shape[-1]
    return jnp.where(lane_mod < half, pltpu.roll(vals, width - half, 1), pltpu.roll(vals, half, 1))


def qkv_kernel(head_dim, x_ref, w_ref, cos_ref, sin_ref, gain_ref, bias_ref, q_ref, k_ref, v_ref):
    blocks, rows, width = x_ref.shape
    normed = norm_rows(x_ref[...].reshape(blocks * rows, width), gain_ref[...], bias_ref[...])
    pair = q_ref.shape[2]
    cos_tab, sin_tab = cos_ref[...], sin_ref[...]
    lane_mod = lax.broadcasted_iota(jnp.int32, cos_tab.shape, 1) % head_dim
    scale = head_dim ** -0.5

    def rotate(vals):
        vals = vals.astype(BF16).astype(F32)
        return (vals * cos_tab + swap_halves(vals, lane_mod, head_dim // 2) * sin_tab).astype(BF16)

    for p in range(0, w_ref.shape[0], 2):
        for h in range(2):
            qk = jnp.dot(normed, w_ref[p + h, :, :2 * pair], preferred_element_type=F32)
            q_ref[p + h] = (rotate(qk[:, :pair]).astype(F32) * scale).astype(BF16)
            k_ref[p + h] = rotate(qk[:, pair:]).astype(F32).T.astype(BF16)
        w_val = jnp.concatenate([w_ref[p, :, 2 * pair:], w_ref[p + 1, :, 2 * pair:]], axis=1)
        vals = jnp.dot(normed, w_val, preferred_element_type=F32).astype(BF16)
        v_ref[p] = vals[:, :pair]
        v_ref[p + 1] = vals[:, pair:]


def attn_kernel(head_dim, rows, chunk, q_ref, k_ref, v_ref, o_ref, s_ref):
    seq, pair = o_ref.shape
    units = [(r, h) for r in range(0, seq, rows) for h in range(pair // head_dim)]
    lane = lax.broadcasted_iota(jnp.int32, (rows, pair), 1)

    def fold(op, vals, carry):
        for t in range(0, vals.shape[1], 128):
            part = vals[:, t:t + 128]
            carry = part if carry is None else op(carry, part)
        return carry

    def load_query(unit):
        r, h = unit
        q = q_ref[0, r:r + rows, :]
        return jnp.where(lane // head_dim == h, q, jnp.zeros_like(q))

    def scores(unit, buf, q, cols, m):
        r, (c, size) = unit[0], cols
        s = jnp.dot(q, k_ref[0, :, c:c + size], preferred_element_type=F32)
        if c + size > r:
            row = lax.broadcasted_iota(jnp.int32, s.shape, 0) + r
            col = lax.broadcasted_iota(jnp.int32, s.shape, 1) + c
            s = jnp.where(col <= row, s, -1e30)
        s_ref[buf, :, c:c + size] = s
        return fold(jnp.maximum, s, m)

    def weigh(buf, m, cols, total, acc):
        c, size = cols
        e = jnp.exp(s_ref[buf, :, c:c + size] - m)
        total = fold(jnp.add, e, total)
        pv = jnp.dot(e.astype(BF16), v_ref[0, c:c + size, :], preferred_element_type=F32)
        return total, pv if acc is None else acc + pv

    def starts(unit):
        end = unit[0] + rows
        return [(c, min(chunk, end - c)) for c in range(0, end, chunk)]

    q_next, m_next = load_query(units[0]), None
    for c in starts(units[0]):
        m_next = scores(units[0], 0, q_next, c, m_next)
    for n, unit in enumerate(units):
        m = jnp.max(m_next, axis=1, keepdims=True)
        total = acc = m_next = None
        follow = units[n + 1] if n + 1 < len(units) else None
        todo = starts(follow) if follow else []
        if follow:
            q_next = load_query(follow)
        for j in range(max(len(todo), len(starts(unit)))):
            if j < len(todo):
                m_next = scores(follow, (n + 1) % 2, q_next, todo[j], m_next)
            if j < len(starts(unit)):
                total, acc = weigh(n % 2, m, starts(unit)[j], total, acc)
        r, h = unit
        out = (acc / jnp.sum(total, axis=1, keepdims=True)).astype(BF16)
        o_ref[r:r + rows, h * head_dim:(h + 1) * head_dim] = out[:, h * head_dim:(h + 1) * head_dim]


def mlp_kernel(sub, x_ref, gain_ref, bias_ref, up_ref, down_ref, o_ref, m_ref, acc_ref):
    f, t = pl.program_id(0), pl.program_id(1)
    rows, width = x_ref.shape
    shards, ff = up_ref.shape[0], up_ref.shape[2]
    base = pl.multiple_of(t * rows, rows)

    @pl.when(f == 0)
    def _():
        for h in range(0, rows, sub):
            part = pl.ds(base + h, sub)
            m_ref[part, :] = norm_rows(x_ref[h:h + sub, :], gain_ref[...], bias_ref[...])
            acc_ref[part, :] = jnp.zeros((sub, width), F32)

    down_w = down_ref[...].reshape(shards * ff, width)

    def expand(h):
        rows_in = m_ref[pl.ds(base + h, sub), :]
        return [jnp.dot(rows_in, up_ref[k], preferred_element_type=F32) for k in range(shards)]

    def gelu(pre):
        return (0.5 * pre * (1.0 + lax.erf(pre * (0.5 ** 0.5)))).astype(BF16)

    pre = expand(0)
    for h in range(0, rows, sub):
        following = expand(h + sub) if h + sub < rows else None
        act = jnp.concatenate([gelu(p) for p in pre], axis=1)
        acc_ref[pl.ds(base + h, sub), :] += jnp.dot(act, down_w, preferred_element_type=F32)
        pre = following

    @pl.when(f == pl.num_programs(0) - 1)
    def _():
        o_ref[...] = acc_ref[pl.ds(base, rows), :]


def final_kernel(x_ref, ctx_ref, wo_ref, mlp_ref, y_ref):
    attn = jnp.dot(ctx_ref[...], wo_ref[...], preferred_element_type=F32)
    y_ref[...] = (x_ref[...].astype(F32) + attn + mlp_ref[...]).astype(BF16)


def params(sem):
    return pltpu.CompilerParams(dimension_semantics=sem, vmem_limit_bytes=VMEM_LIMIT)


def solution(mesh):
    tp = mesh.shape['tp']

    def local_layer(x, attn_gain, attn_bias, mlp_gain, mlp_bias, w_qkv, w_out, w_up, w_down, positions):
        batch, chunk, width = x.shape
        per_dev = batch // tp
        groups, slot_cols = w_qkv.shape[1:]
        ctx_cols = w_out.shape[0]
        head_dim = (slot_cols - ctx_cols // groups) // 2
        pair = groups * head_dim
        seq = chunk * tp
        ff = w_up.shape[1]
        tokens = batch * chunk
        half = head_dim // 2

        w_qkv = w_qkv.reshape(width, groups, 3, head_dim).swapaxes(1, 2).reshape(width, 3 * pair)
        wqkv_all = lax.all_gather(w_qkv, 'tp', axis=0, tiled=False)
        x_seq = lax.all_to_all(x, 'tp', split_axis=0, concat_axis=0, tiled=True)
        x_seq = x_seq.reshape(tp, chunk, width)

        inv_freq = 10000.0 ** (-2.0 * jnp.arange(half, dtype=F32) / head_dim)
        inv_freq = jnp.tile(inv_freq, 2 * groups)
        angles = positions.astype(F32)[:, None] * inv_freq[None, :]
        sign = jnp.where(jnp.arange(pair) % head_dim < half, -1.0, 1.0).astype(F32)
        cos_tab, sin_tab = jnp.cos(angles), jnp.sin(angles) * sign[None, :]

        gain2, bias2 = attn_gain.reshape(1, width), attn_bias.reshape(1, width)
        nb = 2
        q, k, v = pl.pallas_call(
            functools.partial(qkv_kernel, head_dim),
            grid=(tp // nb,),
            in_specs=[
                pl.BlockSpec((nb, chunk, width), lambda i: (i, 0, 0)),
                pl.BlockSpec((tp, width, 3 * pair), lambda i: (0, 0, 0)),
                pl.BlockSpec((nb * chunk, pair), lambda i: (i, 0)),
                pl.BlockSpec((nb * chunk, pair), lambda i: (i, 0)),
                pl.BlockSpec((1, width), lambda i: (0, 0)),
                pl.BlockSpec((1, width), lambda i: (0, 0)),
            ],
            out_specs=[
                pl.BlockSpec((tp, nb * chunk, pair), lambda i: (0, i, 0)),
                pl.BlockSpec((tp, pair, nb * chunk), lambda i: (0, 0, i)),
                pl.BlockSpec((tp, nb * chunk, pair), lambda i: (0, i, 0)),
            ],
            out_shape=[
                jax.ShapeDtypeStruct((tp, seq, pair), BF16),
                jax.ShapeDtypeStruct((tp, pair, seq), BF16),
                jax.ShapeDtypeStruct((tp, seq, pair), BF16),
            ],
            compiler_params=params(('arbitrary',)),
            cost_estimate=pl.CostEstimate(flops=2 * seq * width * 3 * pair * tp, bytes_accessed=2 * (seq * width * 4 + width * 3 * pair * tp), transcendentals=0),
            name='qkv',
        )(x_seq, wqkv_all, cos_tab, sin_tab, gain2, bias2)

        q_rows, kv_cols = 256, 512
        ctx = pl.pallas_call(
            functools.partial(attn_kernel, head_dim, q_rows, kv_cols),
            grid=(tp,),
            in_specs=[
                pl.BlockSpec((1, seq, pair), lambda p: (p, 0, 0)),
                pl.BlockSpec((1, pair, seq), lambda p: (p, 0, 0)),
                pl.BlockSpec((1, seq, pair), lambda p: (p, 0, 0)),
            ],
            out_specs=pl.BlockSpec((seq, pair), lambda p: (0, p)),
            out_shape=jax.ShapeDtypeStruct((seq, tp * pair), BF16),
            scratch_shapes=[pltpu.VMEM((2, q_rows, seq), F32)],
            compiler_params=params(('arbitrary',)),
            cost_estimate=pl.CostEstimate(flops=8 * seq * seq * pair * tp, bytes_accessed=2 * seq * width * 4, transcendentals=0),
            name='attn',
        )(q, k, v)

        w_up, w_down, w_out, _, _ = lax.optimization_barrier((w_up, w_down, w_out, wqkv_all, x_seq))
        up_all = lax.all_gather(w_up, 'tp', axis=0, tiled=False)
        down_all = lax.all_gather(w_down, 'tp', axis=0, tiled=False)
        wo_all = lax.all_gather(w_out, 'tp', axis=0, tiled=True)
        x_mlp, ctx = lax.optimization_barrier((x, ctx))
        ctx_own = lax.all_to_all(ctx.reshape(tp, chunk, width), 'tp', split_axis=0, concat_axis=0, tiled=True)
        x_rows = x_mlp.reshape(tokens, width)
        rows, shards = 1024, 2
        nt, nf = tokens // rows, tp // shards
        mlp = pl.pallas_call(
            functools.partial(mlp_kernel, 256),
            grid=(nf, nt),
            in_specs=[
                pl.BlockSpec((rows, width), lambda f, t: (jnp.where(f == 0, t, nt - 1), 0)),
                pl.BlockSpec((1, width), lambda f, t: (0, 0)),
                pl.BlockSpec((1, width), lambda f, t: (0, 0)),
                pl.BlockSpec((shards, width, ff), lambda f, t: (f, 0, 0)),
                pl.BlockSpec((shards, ff, width), lambda f, t: (f, 0, 0)),
            ],
            out_specs=pl.BlockSpec((rows, width), lambda f, t: (jnp.where(f == nf - 1, t, 0), 0)),
            out_shape=jax.ShapeDtypeStruct((tokens, width), F32),
            scratch_shapes=[pltpu.VMEM((tokens, width), BF16), pltpu.VMEM((tokens, width), F32)],
            compiler_params=params(('arbitrary', 'arbitrary')),
            cost_estimate=pl.CostEstimate(flops=4 * tokens * width * ff * tp, bytes_accessed=4 * tokens * width * 2, transcendentals=0),
            name='mlp',
        )(x_rows, mlp_gain.reshape(1, width), mlp_bias.reshape(1, width), up_all, down_all)

        rows = 512
        nt = tokens // rows
        y = pl.pallas_call(
            final_kernel,
            grid=(nt,),
            in_specs=[
                pl.BlockSpec((rows, width), lambda t: (t, 0)),
                pl.BlockSpec((rows, width), lambda t: (t, 0)),
                pl.BlockSpec((width, width), lambda t: (0, 0)),
                pl.BlockSpec((rows, width), lambda t: (t, 0)),
            ],
            out_specs=pl.BlockSpec((rows, width), lambda t: (t, 0)),
            out_shape=jax.ShapeDtypeStruct((tokens, width), BF16),
            compiler_params=params(('arbitrary',)),
            cost_estimate=pl.CostEstimate(flops=2 * tokens * width * width, bytes_accessed=tokens * width * 10, transcendentals=0),
            name='final',
        )(x_rows, ctx_own.reshape(tokens, width), wo_all, mlp)
        return y.reshape(batch, chunk, width)

    return jax.shard_map(local_layer, mesh=mesh, in_specs=(P('dp', 'tp', None), P(), P(), P(), P(), P(None, 'tp', None), P('tp', None), P(None, 'tp'), P('tp', None), P()), out_specs=P('dp', 'tp', None), check_vma=False)
```

```python
import functools

import jax
import jax.numpy as jnp
from jax import lax
from jax.experimental import pallas as pl
from jax.experimental.pallas import tpu as pltpu
from jax.sharding import PartitionSpec as P

BF16 = jnp.bfloat16
F32 = jnp.float32
VMEM_LIMIT = 60 * 1024 * 1024
MESH = pl.DeviceIdType.MESH


def norm_rows(rows, gain, bias):
    rows32 = rows.astype(F32)
    mean = jnp.mean(rows32, axis=-1, keepdims=True)
    centered = rows32 - mean
    var = jnp.mean(centered * centered, axis=-1, keepdims=True)
    return (centered * lax.rsqrt(var + 1e-5) * gain + bias).astype(BF16)


def swap_halves(vals, lane_mod, half):
    width = vals.shape[-1]
    return jnp.where(lane_mod < half, pltpu.roll(vals, width - half, 1), pltpu.roll(vals, half, 1))


def qkv_kernel(head_dim, x_ref, w_ref, cos_ref, sin_ref, gain_ref, bias_ref, q_ref, k_ref, v_ref):
    blocks, rows, width = x_ref.shape
    normed = norm_rows(x_ref[...].reshape(blocks * rows, width), gain_ref[...], bias_ref[...])
    pair = q_ref.shape[2]
    cos_tab, sin_tab = cos_ref[...], sin_ref[...]
    lane_mod = lax.broadcasted_iota(jnp.int32, cos_tab.shape, 1) % head_dim
    scale = head_dim ** -0.5

    def rotate(vals):
        vals = vals.astype(BF16).astype(F32)
        return (vals * cos_tab + swap_halves(vals, lane_mod, head_dim // 2) * sin_tab).astype(BF16)

    for p in range(0, w_ref.shape[0], 2):
        for h in range(2):
            qk = jnp.dot(normed, w_ref[p + h, :, :2 * pair], preferred_element_type=F32)
            q_ref[p + h] = (rotate(qk[:, :pair]).astype(F32) * scale).astype(BF16)
            k_ref[p + h] = rotate(qk[:, pair:]).astype(F32).T.astype(BF16)
        w_val = jnp.concatenate([w_ref[p, :, 2 * pair:], w_ref[p + 1, :, 2 * pair:]], axis=1)
        vals = jnp.dot(normed, w_val, preferred_element_type=F32).astype(BF16)
        v_ref[p] = vals[:, :pair]
        v_ref[p + 1] = vals[:, pair:]


def attn_kernel(head_dim, rows, chunk, q_ref, k_ref, v_ref, ctx_ref, s_ref, o_ref, send, recv, own_sem):
    p, me, tp = pl.program_id(0), lax.axis_index('tp'), ctx_ref.shape[0]
    seq, pair = o_ref.shape[1:]
    tok = seq // tp
    slot = lax.rem(p, 2)

    def ship(step, r):
        to, lane_cols = lax.rem(me + r, tp), pl.ds(pl.multiple_of(step * pair, pair), pair)
        src = o_ref.at[lax.rem(step, 2), pl.ds(pl.multiple_of(to * tok, tok), tok), :]
        return pltpu.make_async_remote_copy(
            src_ref=src, dst_ref=ctx_ref.at[me, :, lane_cols], send_sem=send.at[lax.rem(step, 2), r], recv_sem=recv.at[step, r],
            device_id={'tp': to}, device_id_type=MESH)

    def keep(step):
        lane_cols = pl.ds(pl.multiple_of(step * pair, pair), pair)
        src = o_ref.at[lax.rem(step, 2), pl.ds(pl.multiple_of(me * tok, tok), tok), :]
        return pltpu.make_async_copy(src, ctx_ref.at[me, :, lane_cols], own_sem.at[lax.rem(step, 2)])

    def drain(step):
        for r in range(1, tp):
            ship(step, r).wait_send()
        keep(step).wait()

    @pl.when(p == 0)
    def _():
        barrier = pltpu.get_barrier_semaphore()
        for r in range(1, tp):
            pl.semaphore_signal(barrier, inc=1, device_id={'tp': lax.rem(me + r, tp)}, device_id_type=MESH)
        pl.semaphore_wait(barrier, tp - 1)

    @pl.when(p >= 2)
    def _():
        drain(p - 2)

    units = [(r, h) for r in range(0, seq, rows) for h in range(pair // head_dim)]
    lane = lax.broadcasted_iota(jnp.int32, (rows, pair), 1)

    def fold(op, vals, carry):
        for t in range(0, vals.shape[1], 128):
            part = vals[:, t:t + 128]
            carry = part if carry is None else op(carry, part)
        return carry

    def load_query(unit):
        r, h = unit
        q = q_ref[0, r:r + rows, :]
        return jnp.where(lane // head_dim == h, q, jnp.zeros_like(q))

    def scores(unit, buf, q, cols, m):
        r, (c, size) = unit[0], cols
        s = jnp.dot(q, k_ref[0, :, c:c + size], preferred_element_type=F32)
        if c + size > r:
            row = lax.broadcasted_iota(jnp.int32, s.shape, 0) + r
            col = lax.broadcasted_iota(jnp.int32, s.shape, 1) + c
            s = jnp.where(col <= row, s, -1e30)
        s_ref[buf, :, c:c + size] = s
        return fold(jnp.maximum, s, m)

    def weigh(buf, m, cols, total, acc):
        c, size = cols
        e = jnp.exp(s_ref[buf, :, c:c + size] - m)
        total = fold(jnp.add, e, total)
        pv = jnp.dot(e.astype(BF16), v_ref[0, c:c + size, :], preferred_element_type=F32)
        return total, pv if acc is None else acc + pv

    def starts(unit):
        end = unit[0] + rows
        return [(c, min(chunk, end - c)) for c in range(0, end, chunk)]

    q_next, m_next = load_query(units[0]), None
    for c in starts(units[0]):
        m_next = scores(units[0], 0, q_next, c, m_next)
    for n, unit in enumerate(units):
        m = jnp.max(m_next, axis=1, keepdims=True)
        total = acc = m_next = None
        follow = units[n + 1] if n + 1 < len(units) else None
        todo = starts(follow) if follow else []
        if follow:
            q_next = load_query(follow)
        for j in range(max(len(todo), len(starts(unit)))):
            if j < len(todo):
                m_next = scores(follow, (n + 1) % 2, q_next, todo[j], m_next)
            if j < len(starts(unit)):
                total, acc = weigh(n % 2, m, starts(unit)[j], total, acc)
        r, h = unit
        out = (acc / jnp.sum(total, axis=1, keepdims=True)).astype(BF16)
        o_ref[slot, r:r + rows, h * head_dim:(h + 1) * head_dim] = out[:, h * head_dim:(h + 1) * head_dim]

    for r in range(1, tp):
        ship(p, r).start()
    keep(p).start()

    @pl.when(p == pl.num_programs(0) - 1)
    def _():
        drain(p - 1)
        drain(p)
        for step in range(recv.shape[0]):
            for r in range(1, tp):
                ship(step, r).wait_recv()


def exchange_kernel(sub, x_ref, gain_ref, bias_ref, up_ref, down_ref, wqkv_ref, wo_ref,
                    xs_ref, wqkv_all, wo_all, acc_ref, up_all, down_all, m_ref, send, recv, xsend, xrecv, own_sem):
    me, tp = lax.axis_index('tp'), xs_ref.shape[0]
    dp = lax.axis_index('dp')
    hz = lax.rem(dp, 2)
    twin = dp + 1 - 2 * hz
    core = lax.rem(me, 2)
    sib = me + 1 - 2 * core
    right, left, far = lax.rem(me + 2, tp), lax.rem(me + tp - 2, tp), lax.rem(me + 4, tp)
    tokens, width = acc_ref.shape

    barrier = pltpu.get_barrier_semaphore()
    for r in range(1, tp):
        pl.semaphore_signal(barrier, inc=1, device_id={'tp': lax.rem(me + r, tp)}, device_id_type=MESH)
    pl.semaphore_signal(barrier, inc=1, device_id={'dp': twin}, device_id_type=MESH)
    pl.semaphore_wait(barrier, tp)

    weights = ((up_ref, up_all, True), (down_ref, down_all, True), (wqkv_ref, wqkv_all, False), (wo_ref, wo_all, True))
    UP, DOWN, QKV, OUT = range(4)

    def whole(ref, shared):
        return ref.at[hz] if shared else ref

    def link(w, k):
        own, every, shared = weights[w]
        rows = own.shape[1]

        def part(s):
            return whole(every.at[s], shared)

        def quarter(s, n):
            if shared:
                return every.at[s, hz, n * (rows // 2):(n + 1) * (rows // 2), :]
            return every.at[s, n]

        if k == 0:
            src, dst, dev = whole(own, shared), part(me), {'tp': right}
        elif k == 1:
            src, dst, dev = whole(own, shared), part(me), {'tp': left}
        elif k == 2:
            src, dst, dev = own, every.at[me], {'tp': sib}
        elif k == 3:
            src, dst, dev = quarter(left, 0), quarter(left, 0), {'tp': right}
        elif k == 4:
            src, dst, dev = quarter(right, 1), quarter(right, 1), {'tp': left}
        elif k < 8:
            s = (left, right, far)[k - 5]
            src, dst, dev = part(s), part(s), {'dp': twin}
        elif k < 11:
            s = (left, right, far)[k - 8]
            src, dst, dev = part(s), part(s), {'tp': sib}
        else:
            s = (left, right, far)[k - 11]
            src, dst, dev = every.at[s, 1 - hz], every.at[s, 1 - hz], {'tp': sib}
        return pltpu.make_async_remote_copy(src_ref=src, dst_ref=dst, send_sem=send.at[w, k], recv_sem=recv.at[w, k], device_id=dev, device_id_type=MESH)

    started = []

    def go(w, *kinds):
        for k in kinds:
            link(w, k).start()
            started.append((w, k))

    def arrived(w, *kinds):
        for k in kinds:
            link(w, k).wait_recv()

    def near(w):
        shared = weights[w][2]
        arrived(w, 0, 1)
        go(w, 3, 4)
        if shared:
            go(w, 5, 6)
        go(w, 8, 9)

    def distant(w):
        shared = weights[w][2]
        arrived(w, 3, 4)
        if shared:
            go(w, 7)
        go(w, 10)

    def token_block(r):
        to = lax.rem(me + r, tp)
        return pltpu.make_async_remote_copy(src_ref=x_ref.at[to], dst_ref=xs_ref.at[me], send_sem=xsend.at[r], recv_sem=xrecv.at[r], device_id={'tp': to}, device_id_type=MESH)

    def gelu(pre):
        return (0.5 * pre * (1.0 + lax.erf(pre * (0.5 ** 0.5)))).astype(BF16)

    def mlp(first, parts):
        ups = [p[0] for p in parts]
        downs = [p[1] for p in parts]

        def body(t, carry):
            base = pl.multiple_of(t * 2 * sub, 2 * sub)

            def expand(h):
                rows_in = m_ref[pl.ds(base + h * sub, sub), :]
                return [jnp.dot(rows_in, u[...], preferred_element_type=F32) for u in ups]

            pre = expand(0)
            for h in range(2):
                following = expand(1) if h == 0 else None
                act = jnp.concatenate([gelu(p) for p in pre], axis=1)
                down_w = jnp.concatenate([d[...] for d in downs], axis=0)
                out = jnp.dot(act, down_w, preferred_element_type=F32)
                rows_out = pl.ds(base + h * sub, sub)
                if first:
                    acc_ref[rows_out, :] = out
                else:
                    acc_ref[rows_out, :] += out
                pre = following
            return carry

        lax.fori_loop(0, tokens // (2 * sub), body, 0)

    def halves(s, n):
        return up_all.at[s, n], down_all.at[s, n]

    local = [
        pltpu.make_async_copy(wqkv_ref, wqkv_all.at[me], own_sem.at[0]),
        pltpu.make_async_copy(wo_ref, wo_all.at[me], own_sem.at[1]),
        pltpu.make_async_copy(x_ref.at[me], xs_ref.at[me], own_sem.at[2]),
    ]
    for w in (UP, DOWN, QKV, OUT):
        go(w, 0, 1, 2)
    for copy in local:
        copy.start()

    def norm(t, carry):
        tok = x_ref.shape[1]
        m_ref[pl.ds(pl.multiple_of(t * tok, tok), tok), :] = norm_rows(x_ref[t], gain_ref[...], bias_ref[...])
        return carry

    lax.fori_loop(0, tp, norm, 0)
    arrived(UP, 2)
    arrived(DOWN, 2)
    near(UP)
    mlp(True, [(up_ref.at[0], down_ref.at[0]), (up_ref.at[1], down_ref.at[1]), halves(sib, 0), halves(sib, 1)])
    near(DOWN)
    distant(UP)
    near(OUT)
    arrived(UP, 8, 9)
    arrived(DOWN, 8, 9)
    sib_left, sib_right, sib_far = left + 1 - 2 * core, right + 1 - 2 * core, far + 1 - 2 * core
    near(QKV)
    for r in range(1, tp):
        token_block(r).start()
    mlp(False, [halves(left, hz), halves(right, hz), halves(sib_left, hz), halves(sib_right, hz)])
    distant(DOWN)
    distant(OUT)
    distant(QKV)
    for w in (UP, DOWN):
        arrived(w, 5, 6)
        go(w, 11, 12)
    arrived(UP, 11, 12)
    arrived(DOWN, 11, 12)
    mlp(False, [halves(left, 1 - hz), halves(right, 1 - hz), halves(sib_left, 1 - hz), halves(sib_right, 1 - hz)])
    for w in (UP, DOWN):
        arrived(w, 7)
        go(w, 13)
    for w in (UP, DOWN):
        arrived(w, 10, 13)
    mlp(False, [halves(far, hz), halves(far, 1 - hz), halves(sib_far, hz), halves(sib_far, 1 - hz)])
    arrived(OUT, 5, 6, 7)
    go(OUT, 11, 12, 13)
    arrived(QKV, 2, 8, 9, 10)
    arrived(OUT, 2, 8, 9, 10, 11, 12, 13)
    for r in range(1, tp):
        token_block(r).wait_recv()
    for w, k in started:
        link(w, k).wait_send()
    for r in range(1, tp):
        token_block(r).wait_send()
    for copy in local:
        copy.wait()


def final_kernel(x_ref, ctx_ref, wo_ref, mlp_ref, y_ref):
    attn = jnp.dot(ctx_ref[...], wo_ref[...], preferred_element_type=F32)
    y_ref[...] = (x_ref[...].astype(F32) + attn + mlp_ref[...]).astype(BF16)


def params(sem):
    return pltpu.CompilerParams(dimension_semantics=sem, vmem_limit_bytes=VMEM_LIMIT)


def solution(mesh):
    tp = mesh.shape['tp']

    def local_layer(x, attn_gain, attn_bias, mlp_gain, mlp_bias, w_qkv, w_out, w_up, w_down, positions):
        batch, chunk, width = x.shape
        per_dev = batch // tp
        groups, slot_cols = w_qkv.shape[1:]
        ctx_cols = w_out.shape[0]
        head_dim = (slot_cols - ctx_cols // groups) // 2
        pair = groups * head_dim
        seq = chunk * tp
        ff = w_up.shape[1]
        tokens = batch * chunk
        half = head_dim // 2

        w_qkv = w_qkv.reshape(width, groups, 3, head_dim).swapaxes(1, 2).reshape(width, 3 * pair)
        half_ff = ff // 2
        vmem = pl.BlockSpec(memory_space=pltpu.VMEM)
        hbm = pl.BlockSpec(memory_space=pl.ANY)
        x_seq, wqkv_all, wo_all, mlp = pl.pallas_call(
            functools.partial(exchange_kernel, 256),
            in_specs=[vmem] * 7,
            out_specs=[hbm, hbm, hbm, vmem],
            out_shape=[
                jax.ShapeDtypeStruct((tp, chunk, width), BF16),
                jax.ShapeDtypeStruct((tp, 2, width // 2, 3 * pair), BF16),
                jax.ShapeDtypeStruct((tp, 2, ctx_cols // 2, width), BF16),
                jax.ShapeDtypeStruct((tokens, width), F32),
            ],
            scratch_shapes=[
                pltpu.VMEM((tp, 2, width, half_ff), BF16),
                pltpu.VMEM((tp, 2, half_ff, width), BF16),
                pltpu.VMEM((tokens, width), BF16),
                pltpu.SemaphoreType.DMA((4, 14)),
                pltpu.SemaphoreType.DMA((4, 14)),
                pltpu.SemaphoreType.DMA((tp,)),
                pltpu.SemaphoreType.DMA((tp,)),
                pltpu.SemaphoreType.DMA((3,)),
            ],
            compiler_params=pltpu.CompilerParams(vmem_limit_bytes=VMEM_LIMIT, collective_id=0, has_side_effects=True),
            cost_estimate=pl.CostEstimate(flops=4 * tokens * width * ff * tp, bytes_accessed=4 * tokens * width * 2, transcendentals=0),
            name='exchange',
        )(x, mlp_gain.reshape(1, width), mlp_bias.reshape(1, width),
          w_up.reshape(width, 2, half_ff).swapaxes(0, 1), w_down.reshape(2, half_ff, width),
          w_qkv.reshape(2, width // 2, 3 * pair), w_out.reshape(2, ctx_cols // 2, width))
        wqkv_all = wqkv_all.reshape(tp, width, 3 * pair)
        wo_all = wo_all.reshape(tp * ctx_cols, width)

        inv_freq = 10000.0 ** (-2.0 * jnp.arange(half, dtype=F32) / head_dim)
        inv_freq = jnp.tile(inv_freq, 2 * groups)
        angles = positions.astype(F32)[:, None] * inv_freq[None, :]
        sign = jnp.where(jnp.arange(pair) % head_dim < half, -1.0, 1.0).astype(F32)
        cos_tab, sin_tab = jnp.cos(angles), jnp.sin(angles) * sign[None, :]

        gain2, bias2 = attn_gain.reshape(1, width), attn_bias.reshape(1, width)
        nb = 2
        q, k, v = pl.pallas_call(
            functools.partial(qkv_kernel, head_dim),
            grid=(tp // nb,),
            in_specs=[
                pl.BlockSpec((nb, chunk, width), lambda i: (i, 0, 0)),
                pl.BlockSpec((tp, width, 3 * pair), lambda i: (0, 0, 0)),
                pl.BlockSpec((nb * chunk, pair), lambda i: (i, 0)),
                pl.BlockSpec((nb * chunk, pair), lambda i: (i, 0)),
                pl.BlockSpec((1, width), lambda i: (0, 0)),
                pl.BlockSpec((1, width), lambda i: (0, 0)),
            ],
            out_specs=[
                pl.BlockSpec((tp, nb * chunk, pair), lambda i: (0, i, 0)),
                pl.BlockSpec((tp, pair, nb * chunk), lambda i: (0, 0, i)),
                pl.BlockSpec((tp, nb * chunk, pair), lambda i: (0, i, 0)),
            ],
            out_shape=[
                jax.ShapeDtypeStruct((tp, seq, pair), BF16),
                jax.ShapeDtypeStruct((tp, pair, seq), BF16),
                jax.ShapeDtypeStruct((tp, seq, pair), BF16),
            ],
            compiler_params=params(('arbitrary',)),
            cost_estimate=pl.CostEstimate(flops=2 * seq * width * 3 * pair * tp, bytes_accessed=2 * (seq * width * 4 + width * 3 * pair * tp), transcendentals=0),
            name='qkv',
        )(x_seq, wqkv_all, cos_tab, sin_tab, gain2, bias2)

        q_rows, kv_cols = 256, 512
        ctx = pl.pallas_call(
            functools.partial(attn_kernel, head_dim, q_rows, kv_cols),
            grid=(tp,),
            in_specs=[
                pl.BlockSpec((1, seq, pair), lambda p: (p, 0, 0)),
                pl.BlockSpec((1, pair, seq), lambda p: (p, 0, 0)),
                pl.BlockSpec((1, seq, pair), lambda p: (p, 0, 0)),
            ],
            out_specs=hbm,
            out_shape=jax.ShapeDtypeStruct((tp, chunk, tp * pair), BF16),
            scratch_shapes=[
                pltpu.VMEM((2, q_rows, seq), F32),
                pltpu.VMEM((2, seq, pair), BF16),
                pltpu.SemaphoreType.DMA((2, tp)),
                pltpu.SemaphoreType.DMA((tp, tp)),
                pltpu.SemaphoreType.DMA((2,)),
            ],
            compiler_params=pltpu.CompilerParams(dimension_semantics=('arbitrary',), vmem_limit_bytes=VMEM_LIMIT, collective_id=1, has_side_effects=True),
            cost_estimate=pl.CostEstimate(flops=8 * seq * seq * pair * tp, bytes_accessed=2 * seq * width * 4, transcendentals=0),
            name='attn',
        )(q, k, v)

        x_rows = x.reshape(tokens, width)
        rows = 512
        nt = tokens // rows
        y = pl.pallas_call(
            final_kernel,
            grid=(nt,),
            in_specs=[
                pl.BlockSpec((rows, width), lambda t: (t, 0)),
                pl.BlockSpec((rows, width), lambda t: (t, 0)),
                pl.BlockSpec((width, width), lambda t: (0, 0)),
                pl.BlockSpec((rows, width), lambda t: (t, 0)),
            ],
            out_specs=pl.BlockSpec((rows, width), lambda t: (t, 0)),
            out_shape=jax.ShapeDtypeStruct((tokens, width), BF16),
            compiler_params=params(('arbitrary',)),
            cost_estimate=pl.CostEstimate(flops=2 * tokens * width * width, bytes_accessed=tokens * width * 10, transcendentals=0),
            name='final',
        )(x_rows, ctx.reshape(tokens, width), wo_all, mlp)
        return y.reshape(batch, chunk, width)

    return jax.shard_map(local_layer, mesh=mesh, in_specs=(P('dp', 'tp', None), P(), P(), P(), P(), P(None, 'tp', None), P('tp', None), P(None, 'tp'), P('tp', None), P()), out_specs=P('dp', 'tp', None), check_vma=False)
```

```python
import functools

import jax
import jax.numpy as jnp
from jax import lax
from jax.experimental import pallas as pl
from jax.experimental.pallas import tpu as pltpu
from jax.sharding import PartitionSpec as P

BF16 = jnp.bfloat16
F32 = jnp.float32
VMEM_LIMIT = 60 * 1024 * 1024
MESH = pl.DeviceIdType.MESH


OUTWARD, FORWARD = (0, 1), (7, 8)
SEAT = (0, 8, 1, 4, 2, 5, 3, 6, 7)
DIRECT, LANDING = (0, 1, 2, 3, 4, 5, 6), (2, 3, 4, 5, 6, 7, 8)


class Places:
    def __init__(self, tp):
        self.me = lax.axis_index('tp')
        self.core = lax.rem(self.me, 2)
        self.right, self.left, self.far = lax.rem(self.me + 2, tp), lax.rem(self.me + tp - 2, tp), lax.rem(self.me + 4, tp)
        self.sib = self.other(self.me)
        self.left_sib, self.right_sib, self.far_sib = self.other(self.left), self.other(self.right), self.other(self.far)

    def other(self, device):
        return device + 1 - 2 * self.core

    def route(self, kind):
        me, left, right = self.me, self.left, self.right
        return (
            (right, self.far, None, 0),
            (left, self.far_sib, None, 1),
            (self.sib, self.sib, me, None),
            (right, right, me, None),
            (left, left, me, None),
            (self.right_sib, self.right_sib, me, None),
            (self.left_sib, self.left_sib, me, None),
            (right, None, left, None),
            (self.left_sib, None, right, None),
        )[kind]


def norm_rows(rows, gain, bias):
    rows32 = rows.astype(F32)
    mean = jnp.mean(rows32, axis=-1, keepdims=True)
    centered = rows32 - mean
    var = jnp.mean(centered * centered, axis=-1, keepdims=True)
    return (centered * lax.rsqrt(var + 1e-5) * gain + bias).astype(BF16)


def swap_halves(vals, lane_mod, half):
    width = vals.shape[-1]
    return jnp.where(lane_mod < half, pltpu.roll(vals, width - half, 1), pltpu.roll(vals, half, 1))


def attn_kernel(head_dim, rows, chunk, q_ref, k_ref, v_ref, ctx_ref, s_ref, o_ref, relay_ref, send, recv, own_sem):
    p, tp = pl.program_id(0), ctx_ref.shape[0]
    place = Places(tp)
    me = place.me
    seq, pair = o_ref.shape[1:]
    tok = seq // tp
    slot = lax.rem(p, 2)

    def ship(step, kind):
        to, block, origin, relay = place.route(kind)
        lane_cols = pl.ds(pl.multiple_of(step * pair, pair), pair)
        if kind in FORWARD:
            src = relay_ref.at[step, FORWARD.index(kind)]
        else:
            src = o_ref.at[lax.rem(step, 2), pl.ds(pl.multiple_of(block * tok, tok), tok), :]
        dst = ctx_ref.at[origin, :, lane_cols] if relay is None else relay_ref.at[step, relay]
        return pltpu.make_async_remote_copy(src_ref=src, dst_ref=dst, send_sem=send.at[step, kind], recv_sem=recv.at[step, kind], device_id={'tp': to}, device_id_type=MESH)

    def keep(step):
        lane_cols = pl.ds(pl.multiple_of(step * pair, pair), pair)
        src = o_ref.at[lax.rem(step, 2), pl.ds(pl.multiple_of(me * tok, tok), tok), :]
        return pltpu.make_async_copy(src, ctx_ref.at[me, :, lane_cols], own_sem.at[lax.rem(step, 2)])

    def drain(step):
        for kind in DIRECT:
            ship(step, kind).wait_send()
        keep(step).wait()

    def pass_on(step):
        for out, kind in zip(OUTWARD, FORWARD):
            ship(step, out).wait_recv()
            ship(step, kind).start()

    @pl.when(p == 0)
    def _():
        barrier = pltpu.get_barrier_semaphore()
        for r in range(1, tp):
            pl.semaphore_signal(barrier, inc=1, device_id={'tp': lax.rem(me + r, tp)}, device_id_type=MESH)
        pl.semaphore_wait(barrier, tp - 1)

    @pl.when(p >= 2)
    def _():
        drain(p - 2)

    units = [(r, h) for r in range(0, seq, rows) for h in range(pair // head_dim)]
    lane = lax.broadcasted_iota(jnp.int32, (rows, pair), 1)

    def fold(op, vals, carry):
        for t in range(0, vals.shape[1], 128):
            part = vals[:, t:t + 128]
            carry = part if carry is None else op(carry, part)
        return carry

    def load_query(unit):
        r, h = unit
        q = q_ref[0, r:r + rows, :]
        return jnp.where(lane // head_dim == h, q, jnp.zeros_like(q))

    def scores(unit, buf, q, cols, m):
        r, (c, size) = unit[0], cols
        s = jnp.dot(q, k_ref[0, :, c:c + size], preferred_element_type=F32)
        if c + size > r:
            row = lax.broadcasted_iota(jnp.int32, s.shape, 0) + r
            col = lax.broadcasted_iota(jnp.int32, s.shape, 1) + c
            s = jnp.where(col <= row, s, -1e30)
        s_ref[buf, :, c:c + size] = s
        return fold(jnp.maximum, s, m)

    def weigh(buf, m, cols, total, acc):
        c, size = cols
        e = jnp.exp(s_ref[buf, :, c:c + size] - m)
        total = fold(jnp.add, e, total)
        pv = jnp.dot(e.astype(BF16), v_ref[0, c:c + size, :], preferred_element_type=F32)
        return total, pv if acc is None else acc + pv

    def starts(unit):
        end = unit[0] + rows
        return [(c, min(chunk, end - c)) for c in range(0, end, chunk)]

    q_next, m_next = load_query(units[0]), None
    for c in starts(units[0]):
        m_next = scores(units[0], 0, q_next, c, m_next)
    for n, unit in enumerate(units):
        m = jnp.max(m_next, axis=1, keepdims=True)
        total = acc = m_next = None
        follow = units[n + 1] if n + 1 < len(units) else None
        todo = starts(follow) if follow else []
        if follow:
            q_next = load_query(follow)
        for j in range(max(len(todo), len(starts(unit)))):
            if j < len(todo):
                m_next = scores(follow, (n + 1) % 2, q_next, todo[j], m_next)
            if j < len(starts(unit)):
                total, acc = weigh(n % 2, m, starts(unit)[j], total, acc)
        r, h = unit
        out = (acc / jnp.sum(total, axis=1, keepdims=True)).astype(BF16)
        o_ref[slot, r:r + rows, h * head_dim:(h + 1) * head_dim] = out[:, h * head_dim:(h + 1) * head_dim]

    for kind in DIRECT:
        ship(p, kind).start()
    keep(p).start()

    @pl.when(p >= 1)
    def _():
        pass_on(p - 1)

    @pl.when(p == pl.num_programs(0) - 1)
    def _():
        pass_on(p)
        drain(p - 1)
        drain(p)
        for step in range(recv.shape[0]):
            for kind in FORWARD:
                ship(step, kind).wait_send()
            for kind in LANDING:
                ship(step, kind).wait_recv()


def exchange_kernel(sub, head_dim, x_ref, mgain_ref, mbias_ref, again_ref, abias_ref, up_ref, down_ref, wqkv_ref, wo_ref, cos4_ref, sin4_ref,
                    q_ref, k_ref, v_ref, wo_all, mlp_ref,
                    xs_ref, wqkv_all, up_all, down_all, m_ref, acc_ref, relay_ref, cos_ref, sin_ref, q_st, k_st, v_st,
                    send, recv, xsend, xrecv, own_sem, out_sem):
    tp = xs_ref.shape[0]
    place = Places(tp)
    me, core, sib = place.me, place.core, place.sib
    right, left, far = place.right, place.left, place.far
    dp = lax.axis_index('dp')
    hz = lax.rem(dp, 2)
    twin = dp + 1 - 2 * hz
    tok = x_ref.shape[1]
    pair = q_ref.shape[2]
    tokens, width = acc_ref.shape

    barrier = pltpu.get_barrier_semaphore()
    for r in range(1, tp):
        pl.semaphore_signal(barrier, inc=1, device_id={'tp': lax.rem(me + r, tp)}, device_id_type=MESH)
    pl.semaphore_signal(barrier, inc=1, device_id={'dp': twin}, device_id_type=MESH)
    pl.semaphore_wait(barrier, tp)

    weights = ((up_ref, up_all, True), (down_ref, down_all, True), (wqkv_ref, wqkv_all, False), (wo_ref, wo_all, True))
    UP, DOWN, QKV, OUT = range(4)

    half_ff = up_all.shape[3]

    def up_cols(n):
        start = n * half_ff
        return up_ref.at[:, pl.ds(start if isinstance(n, int) else pl.multiple_of(start, half_ff), half_ff)]

    def whole(ref, shared):
        return ref.at[hz] if shared else ref

    def link(w, k):
        own, every, shared = weights[w]
        rows = every.shape[2]
        mine = up_cols(hz) if w == UP else whole(own, shared)

        def part(s):
            return whole(every.at[s], shared)

        def quarter(s, n):
            if shared:
                return every.at[s, hz, n * (rows // 2):(n + 1) * (rows // 2), :]
            return every.at[s, n]

        if k == 0:
            src, dst, dev = mine, part(me), {'tp': right}
        elif k == 1:
            src, dst, dev = mine, part(me), {'tp': left}
        elif k == 2:
            src, dst, dev = (up_cols(0), every.at[me, 0], {'tp': sib}) if w == UP else (own, every.at[me], {'tp': sib})
        elif k == 14:
            src, dst, dev = up_cols(1), every.at[me, 1], {'tp': sib}
        elif k == 3:
            src, dst, dev = quarter(left, 0), quarter(left, 0), {'tp': right}
        elif k == 4:
            src, dst, dev = quarter(right, 1), quarter(right, 1), {'tp': left}
        elif k < 8:
            s = (left, right, far)[k - 5]
            src, dst, dev = part(s), part(s), {'dp': twin}
        elif k < 11:
            s = (left, right, far)[k - 8]
            src, dst, dev = part(s), part(s), {'tp': sib}
        else:
            s = (left, right, far)[k - 11]
            src, dst, dev = every.at[s, 1 - hz], every.at[s, 1 - hz], {'tp': sib}
        return pltpu.make_async_remote_copy(src_ref=src, dst_ref=dst, send_sem=send.at[w, k], recv_sem=recv.at[w, k], device_id=dev, device_id_type=MESH)

    started = []

    def go(w, *kinds):
        for k in kinds:
            link(w, k).start()
            started.append((w, k))

    def arrived(w, *kinds):
        for k in kinds:
            link(w, k).wait_recv()

    def near(w):
        shared = weights[w][2]
        arrived(w, 0, 1)
        go(w, 3, 4)
        if shared:
            go(w, 5, 6)
        go(w, 8, 9)

    def distant(w):
        shared = weights[w][2]
        arrived(w, 3, 4)
        if shared:
            go(w, 7)
        go(w, 10)

    def token_block(kind):
        to, block, origin, relay = place.route(kind)
        src = relay_ref.at[FORWARD.index(kind)] if kind in FORWARD else x_ref.at[block]
        dst = xs_ref.at[origin] if relay is None else relay_ref.at[relay]
        return pltpu.make_async_remote_copy(src_ref=src, dst_ref=dst, send_sem=xsend.at[kind], recv_sem=xrecv.at[SEAT[kind]], device_id={'tp': to}, device_id_type=MESH)

    def tables(j):
        quarter = cos4_ref.shape[1] // 4
        lane4 = lax.broadcasted_iota(jnp.int32, cos4_ref.shape, 1)
        rows_j = slice(j * cos4_ref.shape[0], (j + 1) * cos4_ref.shape[0])
        sign = jnp.where(lane4 % head_dim < quarter, -1.0, 1.0).astype(F32)
        for src, dst, factor in ((cos4_ref, cos_ref, None), (sin4_ref, sin_ref, sign)):
            vals = jnp.where(lane4 // quarter == j, src[...], 0.0)
            vals = vals + pltpu.roll(vals, quarter, 1)
            vals = vals + pltpu.roll(vals, 2 * quarter, 1)
            dst[rows_j, :] = vals if factor is None else vals * factor

    def outputs(n):
        block = lax.rem(n, 2)
        at = pl.ds(pl.multiple_of(source(n) * tok, tok), tok)
        return [
            pltpu.make_async_copy(q_st.at[block], q_ref.at[:, at, :], out_sem.at[block, 0]),
            pltpu.make_async_copy(k_st.at[block], k_ref.at[:, :, at], out_sem.at[block, 1]),
            pltpu.make_async_copy(v_st.at[block], v_ref.at[:, at, :], out_sem.at[block, 2]),
        ]

    def source(n):
        k = n // 2
        hop = k + (k // 2) * (1 - 2 * (k % 2))
        return lax.rem(me - core + 2 * hop, tp) + core + (n % 2) * (1 - 2 * core)

    def project(direct, n, carry):
        s, block = source(n), lax.rem(n, 2)
        if not direct:
            pltpu.make_async_remote_copy(src_ref=x_ref.at[0], dst_ref=xs_ref.at[s], send_sem=xsend.at[0], recv_sem=xrecv.at[n], device_id={'tp': right}, device_id_type=MESH).wait_recv()
            for copy in outputs(n - 2):
                copy.wait()
        normed = norm_rows(xs_ref[s], again_ref[...], abias_ref[...])
        at = pl.ds(pl.multiple_of(s * tok, tok), tok)
        cos_tab, sin_tab = cos_ref[at, :], sin_ref[at, :]
        lane = lax.broadcasted_iota(jnp.int32, (tok, pair), 1)
        first = lane < head_dim
        lane_mod = lane % head_dim

        def rotate(vals):
            vals = vals.astype(BF16).astype(F32)
            return (vals * cos_tab + swap_halves(vals, lane_mod, head_dim // 2) * sin_tab).astype(BF16).astype(F32)

        for p in range(tp // 2):
            w = jnp.concatenate([wqkv_all[2 * p].reshape(width, 3 * pair), wqkv_all[2 * p + 1].reshape(width, 3 * pair)], axis=1)
            both = jnp.dot(normed, w, preferred_element_type=F32)
            for h in range(2):
                t0, t1, t2 = [both[:, (3 * h + t) * pair:(3 * h + t + 1) * pair] for t in range(3)]
                q_st[block, 2 * p + h] = (rotate(jnp.where(first, t0, t1)) * head_dim ** -0.5).astype(BF16)
                keys = rotate(jnp.where(first, t2, t0)).T.astype(BF16)
                k_st[block, 2 * p + h, :head_dim, :] = keys[head_dim:, :]
                k_st[block, 2 * p + h, head_dim:, :] = keys[:head_dim, :]
                v_st[block, 2 * p + h] = jnp.where(first, t1, t2).astype(BF16)
        for copy in outputs(n):
            copy.start()
        return carry

    def gelu(pre):
        return (0.5 * pre * (1.0 + lax.erf(pre * (0.5 ** 0.5)))).astype(BF16)

    def mlp(first, parts):
        ups = [p[0] for p in parts]
        downs = [p[1] for p in parts]

        def body(t, carry):
            base = pl.multiple_of(t * 2 * sub, 2 * sub)

            def expand(h):
                rows_in = m_ref[pl.ds(base + h * sub, sub), :]
                return [jnp.dot(rows_in, u[...], preferred_element_type=F32) for u in ups]

            pre = expand(0)
            for h in range(2):
                following = expand(1) if h == 0 else None
                act = jnp.concatenate([gelu(p) for p in pre], axis=1)
                down_w = jnp.concatenate([d[...] for d in downs], axis=0)
                out = jnp.dot(act, down_w, preferred_element_type=F32)
                rows_out = pl.ds(base + h * sub, sub)
                if first:
                    acc_ref[rows_out, :] = out
                else:
                    acc_ref[rows_out, :] += out
                pre = following
            return carry

        lax.fori_loop(0, tokens // (2 * sub), body, 0)

    def halves(s, n):
        return up_all.at[s, n], down_all.at[s, n]

    local = pltpu.make_async_copy(wo_ref, wo_all.at[me], own_sem.at[0])
    done = pltpu.make_async_copy(acc_ref, mlp_ref, own_sem.at[1])
    for w in (UP, DOWN, QKV, OUT):
        go(w, 0, 1, 2)
    go(UP, 14)
    local.start()
    token_block(2).start()

    def norm(t, carry):
        m_ref[pl.ds(pl.multiple_of(t * tok, tok), tok), :] = norm_rows(x_ref[t], mgain_ref[...], mbias_ref[...])
        return carry

    lax.fori_loop(0, tp, norm, 0)
    arrived(UP, 2, 14)
    arrived(DOWN, 2)
    near(UP)
    mlp(True, [(up_cols(0), down_ref.at[0]), (up_cols(1), down_ref.at[1]), halves(sib, 0), halves(sib, 1)])
    near(DOWN)
    arrived(UP, 8, 9)
    arrived(DOWN, 8, 9)
    left_sib, right_sib, far_sib = place.left_sib, place.right_sib, place.far_sib
    mlp(False, [halves(left, hz), halves(right, hz), halves(left_sib, hz), halves(right_sib, hz)])
    near(OUT)
    near(QKV)
    for kind in (0, 1, 3, 4, 5, 6):
        token_block(kind).start()
    for j in range(4):
        tables(j)
    xs_ref[me] = x_ref[me]
    wqkv_all[me] = wqkv_ref[...]
    distant(UP)
    distant(DOWN)
    for w in (UP, DOWN):
        arrived(w, 5, 6)
        go(w, 11, 12)
    arrived(UP, 11, 12)
    arrived(DOWN, 11, 12)
    mlp(False, [halves(left, 1 - hz), halves(right, 1 - hz), halves(left_sib, 1 - hz), halves(right_sib, 1 - hz)])
    distant(OUT)
    distant(QKV)
    for out, kind in zip(OUTWARD, FORWARD):
        token_block(out).wait_recv()
        token_block(kind).start()
    for w in (UP, DOWN):
        arrived(w, 7)
        go(w, 13)
    arrived(QKV, 2, 8, 9, 10)
    token_block(2).wait_recv()
    lax.fori_loop(0, 2, functools.partial(project, True), 0)
    for w in (UP, DOWN):
        arrived(w, 10, 13)
    mlp(False, [halves(far, hz), halves(far, 1 - hz), halves(far_sib, hz), halves(far_sib, 1 - hz)])
    done.start()
    arrived(OUT, 5, 6, 7)
    go(OUT, 11, 12, 13)
    lax.fori_loop(2, tp, functools.partial(project, False), 0)
    for n in (6, 7):
        for copy in outputs(n):
            copy.wait()
    arrived(OUT, 2, 8, 9, 10, 11, 12, 13)
    for w, k in started:
        link(w, k).wait_send()
    for kind in range(9):
        token_block(kind).wait_send()
    local.wait()
    done.wait()


def final_kernel(x_ref, ctx_ref, wo_ref, mlp_ref, y_ref):
    attn = jnp.dot(ctx_ref[...], wo_ref[...], preferred_element_type=F32)
    y_ref[...] = (x_ref[...].astype(F32) + attn + mlp_ref[...]).astype(BF16)


def params(sem):
    return pltpu.CompilerParams(dimension_semantics=sem, vmem_limit_bytes=VMEM_LIMIT)


def solution(mesh):
    tp = mesh.shape['tp']

    def local_layer(x, attn_gain, attn_bias, mlp_gain, mlp_bias, w_qkv, w_out, w_up, w_down, positions):
        batch, chunk, width = x.shape
        per_dev = batch // tp
        groups, slot_cols = w_qkv.shape[1:]
        ctx_cols = w_out.shape[0]
        head_dim = (slot_cols - ctx_cols // groups) // 2
        pair = groups * head_dim
        seq = chunk * tp
        ff = w_up.shape[1]
        tokens = batch * chunk
        half = head_dim // 2

        inv_freq = 10000.0 ** (-2.0 * jnp.arange(half, dtype=F32) / head_dim)
        reps = pair // half
        pos4 = positions.astype(F32).reshape(reps, seq // reps)
        angles = (pos4.T[:, :, None] * inv_freq[None, None, :]).reshape(seq // reps, pair)
        half_ff = ff // 2
        vmem = pl.BlockSpec(memory_space=pltpu.VMEM)
        hbm = pl.BlockSpec(memory_space=pl.ANY)
        q, k, v, wo_all, mlp = pl.pallas_call(
            functools.partial(exchange_kernel, 256, head_dim),
            in_specs=[vmem] * 11,
            out_specs=[hbm] * 5,
            out_shape=[
                jax.ShapeDtypeStruct((tp, seq, pair), BF16),
                jax.ShapeDtypeStruct((tp, pair, seq), BF16),
                jax.ShapeDtypeStruct((tp, seq, pair), BF16),
                jax.ShapeDtypeStruct((tp, 2, ctx_cols // 2, width), BF16),
                jax.ShapeDtypeStruct((tokens, width), F32),
            ],
            scratch_shapes=[
                pltpu.VMEM((tp, chunk, width), BF16),
                pltpu.VMEM((tp, 2, width // 2, 3 * pair), BF16),
                pltpu.VMEM((tp, 2, width, half_ff), BF16),
                pltpu.VMEM((tp, 2, half_ff, width), BF16),
                pltpu.VMEM((tokens, width), BF16),
                pltpu.VMEM((tokens, width), F32),
                pltpu.VMEM((2, chunk, width), BF16),
                pltpu.VMEM((seq, pair), F32),
                pltpu.VMEM((seq, pair), F32),
                pltpu.VMEM((2, tp, chunk, pair), BF16),
                pltpu.VMEM((2, tp, pair, chunk), BF16),
                pltpu.VMEM((2, tp, chunk, pair), BF16),
                pltpu.SemaphoreType.DMA((4, 15)),
                pltpu.SemaphoreType.DMA((4, 15)),
                pltpu.SemaphoreType.DMA((9,)),
                pltpu.SemaphoreType.DMA((9,)),
                pltpu.SemaphoreType.DMA((2,)),
                pltpu.SemaphoreType.DMA((2, 3)),
            ],
            compiler_params=pltpu.CompilerParams(vmem_limit_bytes=VMEM_LIMIT, collective_id=0, has_side_effects=True),
            cost_estimate=pl.CostEstimate(flops=4 * tokens * width * ff * tp, bytes_accessed=4 * tokens * width * 2, transcendentals=0),
            name='exchange',
        )(x, mlp_gain.reshape(1, width), mlp_bias.reshape(1, width), attn_gain.reshape(1, width), attn_bias.reshape(1, width),
          w_up, w_down.reshape(2, half_ff, width),
          w_qkv.reshape(2, width // 2, 3 * pair), w_out.reshape(2, ctx_cols // 2, width), jnp.cos(angles), jnp.sin(angles))
        wo_all = wo_all.reshape(tp * ctx_cols, width)

        q_rows, kv_cols = 256, 512
        ctx = pl.pallas_call(
            functools.partial(attn_kernel, head_dim, q_rows, kv_cols),
            grid=(tp,),
            in_specs=[
                pl.BlockSpec((1, seq, pair), lambda p: (p, 0, 0)),
                pl.BlockSpec((1, pair, seq), lambda p: (p, 0, 0)),
                pl.BlockSpec((1, seq, pair), lambda p: (p, 0, 0)),
            ],
            out_specs=hbm,
            out_shape=jax.ShapeDtypeStruct((tp, chunk, tp * pair), BF16),
            scratch_shapes=[
                pltpu.VMEM((2, q_rows, seq), F32),
                pltpu.VMEM((2, seq, pair), BF16),
                pltpu.VMEM((tp, 2, chunk, pair), BF16),
                pltpu.SemaphoreType.DMA((tp, 9)),
                pltpu.SemaphoreType.DMA((tp, 9)),
                pltpu.SemaphoreType.DMA((2,)),
            ],
            compiler_params=pltpu.CompilerParams(dimension_semantics=('arbitrary',), vmem_limit_bytes=VMEM_LIMIT, collective_id=1, has_side_effects=True),
            cost_estimate=pl.CostEstimate(flops=8 * seq * seq * pair * tp, bytes_accessed=2 * seq * width * 4, transcendentals=0),
            name='attn',
        )(q, k, v)

        x_rows = x.reshape(tokens, width)
        rows = 512
        nt = tokens // rows
        y = pl.pallas_call(
            final_kernel,
            grid=(nt,),
            in_specs=[
                pl.BlockSpec((rows, width), lambda t: (t, 0)),
                pl.BlockSpec((rows, width), lambda t: (t, 0)),
                pl.BlockSpec((width, width), lambda t: (0, 0)),
                pl.BlockSpec((rows, width), lambda t: (t, 0)),
            ],
            out_specs=pl.BlockSpec((rows, width), lambda t: (t, 0)),
            out_shape=jax.ShapeDtypeStruct((tokens, width), BF16),
            compiler_params=params(('arbitrary',)),
            cost_estimate=pl.CostEstimate(flops=2 * tokens * width * width, bytes_accessed=tokens * width * 10, transcendentals=0),
            name='final',
        )(x_rows, ctx.reshape(tokens, width), wo_all, mlp)
        return y.reshape(batch, chunk, width)

    return jax.shard_map(local_layer, mesh=mesh, in_specs=(P('dp', 'tp', None), P(), P(), P(), P(), P(None, 'tp', None), P('tp', None), P(None, 'tp'), P('tp', None), P()), out_specs=P('dp', 'tp', None), check_vma=False)
```

```python
import functools

import jax
import jax.numpy as jnp
from jax import lax
from jax.experimental import pallas as pl
from jax.experimental.pallas import tpu as pltpu
from jax.sharding import PartitionSpec as P

BF16 = jnp.bfloat16
F32 = jnp.float32
VMEM_LIMIT = 60 * 1024 * 1024
MESH = pl.DeviceIdType.MESH


OUTWARD, FORWARD = (0, 1), (7, 8)
SEAT = (0, 8, 1, 4, 2, 5, 3, 6, 7)
DIRECT, LANDING = (0, 1, 2, 3, 4, 5, 6), (2, 3, 4, 5, 6, 7, 8)


class Places:
    def __init__(self, tp):
        self.me = lax.axis_index('tp')
        self.core = lax.rem(self.me, 2)
        self.right, self.left, self.far = lax.rem(self.me + 2, tp), lax.rem(self.me + tp - 2, tp), lax.rem(self.me + 4, tp)
        self.sib = self.other(self.me)
        self.left_sib, self.right_sib, self.far_sib = self.other(self.left), self.other(self.right), self.other(self.far)

    def other(self, device):
        return device + 1 - 2 * self.core

    def route(self, kind):
        me, left, right = self.me, self.left, self.right
        return (
            (right, self.far, None, 0),
            (left, self.far_sib, None, 1),
            (self.sib, self.sib, me, None),
            (right, right, me, None),
            (left, left, me, None),
            (self.right_sib, self.right_sib, me, None),
            (self.left_sib, self.left_sib, me, None),
            (right, None, left, None),
            (self.left_sib, None, right, None),
        )[kind]


def norm_rows(rows, gain, bias):
    rows32 = rows.astype(F32)
    mean = jnp.mean(rows32, axis=-1, keepdims=True)
    centered = rows32 - mean
    var = jnp.mean(centered * centered, axis=-1, keepdims=True)
    return (centered * lax.rsqrt(var + 1e-5) * gain + bias).astype(BF16)


def swap_halves(vals, lane_mod, half):
    width = vals.shape[-1]
    return jnp.where(lane_mod < half, pltpu.roll(vals, width - half, 1), pltpu.roll(vals, half, 1))


def attn_kernel(head_dim, rows, chunk, q_ref, k_ref, v_ref, ctx_ref, s_ref, o_ref, relay_ref, send, recv, own_sem):
    p, tp = pl.program_id(0), ctx_ref.shape[0]
    place = Places(tp)
    me = place.me
    seq, pair = o_ref.shape[1:]
    tok = seq // tp
    slot = lax.rem(p, 2)

    def ship(step, kind):
        to, block, origin, relay = place.route(kind)
        lane_cols = pl.ds(pl.multiple_of(step * pair, pair), pair)
        if kind in FORWARD:
            src = relay_ref.at[step, FORWARD.index(kind)]
        else:
            src = o_ref.at[lax.rem(step, 2), pl.ds(pl.multiple_of(block * tok, tok), tok), :]
        dst = ctx_ref.at[origin, :, lane_cols] if relay is None else relay_ref.at[step, relay]
        return pltpu.make_async_remote_copy(src_ref=src, dst_ref=dst, send_sem=send.at[step, kind], recv_sem=recv.at[step, kind], device_id={'tp': to}, device_id_type=MESH)

    def keep(step):
        lane_cols = pl.ds(pl.multiple_of(step * pair, pair), pair)
        src = o_ref.at[lax.rem(step, 2), pl.ds(pl.multiple_of(me * tok, tok), tok), :]
        return pltpu.make_async_copy(src, ctx_ref.at[me, :, lane_cols], own_sem.at[lax.rem(step, 2)])

    def drain(step):
        for kind in DIRECT:
            ship(step, kind).wait_send()
        keep(step).wait()

    def send_rows(start):
        for kind in DIRECT:
            mine = place.route(kind)[1] * tok // (seq // 2) == start // (seq // 2)
            pl.when(mine)(ship(p, kind).start)

    def pass_on(step):
        for out, kind in zip(OUTWARD, FORWARD):
            ship(step, out).wait_recv()
            ship(step, kind).start()

    @pl.when(p == 0)
    def _():
        barrier = pltpu.get_barrier_semaphore()
        for r in range(1, tp):
            pl.semaphore_signal(barrier, inc=1, device_id={'tp': lax.rem(me + r, tp)}, device_id_type=MESH)
        pl.semaphore_wait(barrier, tp - 1)

    @pl.when(p >= 2)
    def _():
        drain(p - 2)

    units = [(r, h) for r in range(0, seq, rows) for h in range(pair // head_dim)]
    lane = lax.broadcasted_iota(jnp.int32, (rows, pair), 1)

    def fold(op, vals, carry):
        for t in range(0, vals.shape[1], 128):
            part = vals[:, t:t + 128]
            carry = part if carry is None else op(carry, part)
        return carry

    def load_query(unit):
        r, h = unit
        q = q_ref[0, r:r + rows, :]
        return jnp.where(lane // head_dim == h, q, jnp.zeros_like(q))

    def scores(unit, buf, q, cols, m):
        r, (c, size) = unit[0], cols
        s = jnp.dot(q, k_ref[0, :, c:c + size], preferred_element_type=F32)
        if c + size > r:
            row = lax.broadcasted_iota(jnp.int32, s.shape, 0) + r
            col = lax.broadcasted_iota(jnp.int32, s.shape, 1) + c
            s = jnp.where(col <= row, s, -1e30)
        s_ref[buf, :, c:c + size] = s
        return fold(jnp.maximum, s, m)

    def weigh(buf, m, cols, total, acc):
        c, size = cols
        e = jnp.exp(s_ref[buf, :, c:c + size] - m)
        total = fold(jnp.add, e, total)
        pv = jnp.dot(e.astype(BF16), v_ref[0, c:c + size, :], preferred_element_type=F32)
        return total, pv if acc is None else acc + pv

    def starts(unit):
        end = unit[0] + rows
        return [(c, min(chunk, end - c)) for c in range(0, end, chunk)]

    q_next, m_next = load_query(units[0]), None
    for c in starts(units[0]):
        m_next = scores(units[0], 0, q_next, c, m_next)
    for n, unit in enumerate(units):
        m = jnp.max(m_next, axis=1, keepdims=True)
        total = acc = m_next = None
        follow = units[n + 1] if n + 1 < len(units) else None
        todo = starts(follow) if follow else []
        if follow:
            q_next = load_query(follow)
        for j in range(max(len(todo), len(starts(unit)))):
            if j < len(todo):
                m_next = scores(follow, (n + 1) % 2, q_next, todo[j], m_next)
            if j < len(starts(unit)):
                total, acc = weigh(n % 2, m, starts(unit)[j], total, acc)
        r, h = unit
        out = (acc / jnp.sum(total, axis=1, keepdims=True)).astype(BF16)
        o_ref[slot, r:r + rows, h * head_dim:(h + 1) * head_dim] = out[:, h * head_dim:(h + 1) * head_dim]
        if follow and r < seq // 2 <= follow[0]:
            send_rows(0)

    send_rows(seq // 2)
    keep(p).start()

    @pl.when(p >= 1)
    def _():
        pass_on(p - 1)

    @pl.when(p == pl.num_programs(0) - 1)
    def _():
        pass_on(p)
        drain(p - 1)
        drain(p)
        for step in range(recv.shape[0]):
            for kind in FORWARD:
                ship(step, kind).wait_send()
            for kind in LANDING:
                ship(step, kind).wait_recv()


def exchange_kernel(sub, head_dim, x_ref, mgain_ref, mbias_ref, again_ref, abias_ref, up_ref, down_ref, wqkv_ref, wo_ref, cos4_ref, sin4_ref,
                    q_ref, k_ref, v_ref, wo_all, mlp_ref,
                    xs_ref, wqkv_all, up_all, down_all, m_ref, acc_ref, relay_ref, cos_ref, sin_ref, q_st, k_st, v_st,
                    send, recv, xsend, xrecv, own_sem, out_sem):
    tp = xs_ref.shape[0]
    place = Places(tp)
    me, core, sib = place.me, place.core, place.sib
    right, left, far = place.right, place.left, place.far
    dp = lax.axis_index('dp')
    hz = lax.rem(dp, 2)
    twin = dp + 1 - 2 * hz
    tok = x_ref.shape[1]
    pair = q_ref.shape[2]
    tokens, width = acc_ref.shape

    barrier = pltpu.get_barrier_semaphore()
    for r in range(1, tp):
        pl.semaphore_signal(barrier, inc=1, device_id={'tp': lax.rem(me + r, tp)}, device_id_type=MESH)
    pl.semaphore_signal(barrier, inc=1, device_id={'dp': twin}, device_id_type=MESH)
    pl.semaphore_wait(barrier, tp)

    weights = ((up_ref, up_all, True), (down_ref, down_all, True), (wqkv_ref, wqkv_all, False), (wo_ref, wo_all, True))
    UP, DOWN, QKV, OUT = range(4)

    half_ff = up_all.shape[3]

    def up_cols(n):
        start = n * half_ff
        return up_ref.at[:, pl.ds(start if isinstance(n, int) else pl.multiple_of(start, half_ff), half_ff)]

    def whole(ref, shared):
        return ref.at[hz] if shared else ref

    def link(w, k):
        own, every, shared = weights[w]
        rows = every.shape[2]
        mine = up_cols(hz) if w == UP else whole(own, shared)

        def part(s):
            return whole(every.at[s], shared)

        def quarter(s, n):
            if shared:
                return every.at[s, hz, n * (rows // 2):(n + 1) * (rows // 2), :]
            return every.at[s, n]

        if k == 0:
            src, dst, dev = mine, part(me), {'tp': right}
        elif k == 1:
            src, dst, dev = mine, part(me), {'tp': left}
        elif k == 2:
            src, dst, dev = (up_cols(0), every.at[me, 0], {'tp': sib}) if w == UP else (own, every.at[me], {'tp': sib})
        elif k == 14:
            src, dst, dev = up_cols(1), every.at[me, 1], {'tp': sib}
        elif k == 3:
            src, dst, dev = quarter(left, 0), quarter(left, 0), {'tp': right}
        elif k == 4:
            src, dst, dev = quarter(right, 1), quarter(right, 1), {'tp': left}
        elif k < 8:
            s = (left, right, far)[k - 5]
            src, dst, dev = part(s), part(s), {'dp': twin}
        elif k < 11:
            s = (left, right, far)[k - 8]
            src, dst, dev = part(s), part(s), {'tp': sib}
        else:
            s = (left, right, far)[k - 11]
            src, dst, dev = every.at[s, 1 - hz], every.at[s, 1 - hz], {'tp': sib}
        return pltpu.make_async_remote_copy(src_ref=src, dst_ref=dst, send_sem=send.at[w, k], recv_sem=recv.at[w, k], device_id=dev, device_id_type=MESH)

    started = []

    def go(w, *kinds):
        for k in kinds:
            link(w, k).start()
            started.append((w, k))

    def arrived(w, *kinds):
        for k in kinds:
            link(w, k).wait_recv()

    def near(w):
        shared = weights[w][2]
        arrived(w, 0, 1)
        go(w, 3, 4)
        if shared:
            go(w, 5, 6)
        go(w, 8, 9)

    def distant(w):
        shared = weights[w][2]
        arrived(w, 3, 4)
        if shared:
            go(w, 7)
        go(w, 10)

    def token_block(kind):
        to, block, origin, relay = place.route(kind)
        src = relay_ref.at[FORWARD.index(kind)] if kind in FORWARD else x_ref.at[block]
        dst = xs_ref.at[origin] if relay is None else relay_ref.at[relay]
        return pltpu.make_async_remote_copy(src_ref=src, dst_ref=dst, send_sem=xsend.at[kind], recv_sem=xrecv.at[SEAT[kind]], device_id={'tp': to}, device_id_type=MESH)

    def tables(j):
        quarter = cos4_ref.shape[1] // 4
        lane4 = lax.broadcasted_iota(jnp.int32, cos4_ref.shape, 1)
        rows_j = slice(j * cos4_ref.shape[0], (j + 1) * cos4_ref.shape[0])
        sign = jnp.where(lane4 % head_dim < quarter, -1.0, 1.0).astype(F32)
        for src, dst, factor in ((cos4_ref, cos_ref, None), (sin4_ref, sin_ref, sign)):
            vals = jnp.where(lane4 // quarter == j, src[...], 0.0)
            vals = vals + pltpu.roll(vals, quarter, 1)
            vals = vals + pltpu.roll(vals, 2 * quarter, 1)
            dst[rows_j, :] = vals if factor is None else vals * factor

    def outputs(n):
        block = lax.rem(n, 2)
        at = pl.ds(pl.multiple_of(source(n) * tok, tok), tok)
        return [
            pltpu.make_async_copy(q_st.at[block], q_ref.at[:, at, :], out_sem.at[block, 0]),
            pltpu.make_async_copy(k_st.at[block], k_ref.at[:, :, at], out_sem.at[block, 1]),
            pltpu.make_async_copy(v_st.at[block], v_ref.at[:, at, :], out_sem.at[block, 2]),
        ]

    def source(n):
        k = n // 2
        hop = k + (k // 2) * (1 - 2 * (k % 2))
        return lax.rem(me - core + 2 * hop, tp) + core + (n % 2) * (1 - 2 * core)

    def project(direct, n, carry):
        s, block = source(n), lax.rem(n, 2)
        if not direct:
            pltpu.make_async_remote_copy(src_ref=x_ref.at[0], dst_ref=xs_ref.at[s], send_sem=xsend.at[0], recv_sem=xrecv.at[n], device_id={'tp': right}, device_id_type=MESH).wait_recv()
            for copy in outputs(n - 2):
                copy.wait()
        normed = norm_rows(xs_ref[s], again_ref[...], abias_ref[...])
        at = pl.ds(pl.multiple_of(s * tok, tok), tok)
        cos_tab, sin_tab = cos_ref[at, :], sin_ref[at, :]
        lane = lax.broadcasted_iota(jnp.int32, (tok, pair), 1)
        first = lane < head_dim
        lane_mod = lane % head_dim

        def rotate(vals):
            vals = vals.astype(BF16).astype(F32)
            return (vals * cos_tab + swap_halves(vals, lane_mod, head_dim // 2) * sin_tab).astype(BF16).astype(F32)

        for p in range(tp // 2):
            w = wqkv_all[2 * p:2 * p + 2].reshape(6 * pair, width)
            both = lax.dot_general(normed, w, (((1,), (1,)), ((), ())), preferred_element_type=F32)
            for h in range(2):
                t0, t1, t2 = [both[:, (3 * h + t) * pair:(3 * h + t + 1) * pair] for t in range(3)]
                q_st[block, 2 * p + h] = (rotate(jnp.where(first, t0, t1)) * head_dim ** -0.5).astype(BF16)
                keys = rotate(jnp.where(first, t2, t0)).T.astype(BF16)
                k_st[block, 2 * p + h, :head_dim, :] = keys[head_dim:, :]
                k_st[block, 2 * p + h, head_dim:, :] = keys[:head_dim, :]
                v_st[block, 2 * p + h] = jnp.where(first, t1, t2).astype(BF16)
        for copy in outputs(n):
            copy.start()
        return carry

    def gelu(pre):
        return (0.5 * pre * (1.0 + lax.erf(pre * (0.5 ** 0.5)))).astype(BF16)

    def mlp(first, parts):
        ups = [p[0] for p in parts]
        downs = [p[1] for p in parts]

        def body(t, carry):
            base = pl.multiple_of(t * 2 * sub, 2 * sub)

            def expand(h):
                rows_in = m_ref[pl.ds(base + h * sub, sub), :]
                return [jnp.dot(rows_in, u[...], preferred_element_type=F32) for u in ups]

            pre = expand(0)
            for h in range(2):
                following = expand(1) if h == 0 else None
                act = jnp.concatenate([gelu(p) for p in pre], axis=1)
                down_w = jnp.concatenate([d[...] for d in downs], axis=0)
                out = jnp.dot(act, down_w, preferred_element_type=F32)
                rows_out = pl.ds(base + h * sub, sub)
                if first:
                    acc_ref[rows_out, :] = out + x_ref[2 * t + h].astype(F32)
                else:
                    acc_ref[rows_out, :] += out
                pre = following
            return carry

        lax.fori_loop(0, tokens // (2 * sub), body, 0)

    def halves(s, n):
        return up_all.at[s, n], down_all.at[s, n]

    local = pltpu.make_async_copy(wo_ref, wo_all.at[me], own_sem.at[0])
    done = pltpu.make_async_copy(acc_ref, mlp_ref, own_sem.at[1])
    for w in (UP, DOWN, QKV, OUT):
        go(w, 0, 1, 2)
    go(UP, 14)
    local.start()
    token_block(2).start()

    def norm(t, carry):
        m_ref[pl.ds(pl.multiple_of(t * tok, tok), tok), :] = norm_rows(x_ref[t], mgain_ref[...], mbias_ref[...])
        return carry

    lax.fori_loop(0, tp, norm, 0)
    arrived(UP, 2, 14)
    arrived(DOWN, 2)
    near(UP)
    mlp(True, [(up_cols(0), down_ref.at[0]), (up_cols(1), down_ref.at[1]), halves(sib, 0), halves(sib, 1)])
    near(DOWN)
    arrived(UP, 8, 9)
    arrived(DOWN, 8, 9)
    left_sib, right_sib, far_sib = place.left_sib, place.right_sib, place.far_sib
    mlp(False, [halves(left, hz), halves(right, hz), halves(left_sib, hz), halves(right_sib, hz)])
    near(OUT)
    near(QKV)
    for kind in (0, 1, 3, 4, 5, 6):
        token_block(kind).start()
    for j in range(4):
        tables(j)
    xs_ref[me] = x_ref[me]
    wqkv_all[me] = wqkv_ref[...]
    distant(UP)
    distant(DOWN)
    for w in (UP, DOWN):
        arrived(w, 5, 6)
        go(w, 11, 12)
    arrived(UP, 11, 12)
    arrived(DOWN, 11, 12)
    mlp(False, [halves(left, 1 - hz), halves(right, 1 - hz), halves(left_sib, 1 - hz), halves(right_sib, 1 - hz)])
    distant(OUT)
    distant(QKV)
    for out, kind in zip(OUTWARD, FORWARD):
        token_block(out).wait_recv()
        token_block(kind).start()
    for w in (UP, DOWN):
        arrived(w, 7)
        go(w, 13)
    arrived(QKV, 2, 8, 9, 10)
    token_block(2).wait_recv()
    lax.fori_loop(0, 2, functools.partial(project, True), 0)
    for w in (UP, DOWN):
        arrived(w, 10, 13)
    mlp(False, [halves(far, hz), halves(far, 1 - hz), halves(far_sib, hz), halves(far_sib, 1 - hz)])
    done.start()
    arrived(OUT, 5, 6, 7)
    go(OUT, 11, 12, 13)
    lax.fori_loop(2, tp, functools.partial(project, False), 0)
    for n in (6, 7):
        for copy in outputs(n):
            copy.wait()
    arrived(OUT, 2, 8, 9, 10, 11, 12, 13)
    for w, k in started:
        link(w, k).wait_send()
    for kind in range(9):
        token_block(kind).wait_send()
    local.wait()
    done.wait()


def final_kernel(ctx_ref, wo_ref, rest_ref, y_ref):
    attn = jnp.dot(ctx_ref[...], wo_ref[...], preferred_element_type=F32)
    y_ref[...] = (rest_ref[...] + attn).astype(BF16)


def params(sem):
    return pltpu.CompilerParams(dimension_semantics=sem, vmem_limit_bytes=VMEM_LIMIT)


def solution(mesh):
    tp = mesh.shape['tp']

    def local_layer(x, attn_gain, attn_bias, mlp_gain, mlp_bias, w_qkv, w_out, w_up, w_down, positions):
        batch, chunk, width = x.shape
        per_dev = batch // tp
        groups, slot_cols = w_qkv.shape[1:]
        ctx_cols = w_out.shape[0]
        head_dim = (slot_cols - ctx_cols // groups) // 2
        pair = groups * head_dim
        seq = chunk * tp
        ff = w_up.shape[1]
        tokens = batch * chunk
        half = head_dim // 2

        inv_freq = 10000.0 ** (-2.0 * jnp.arange(half, dtype=F32) / head_dim)
        reps = pair // half
        pos4 = positions.astype(F32).reshape(reps, seq // reps)
        angles = (pos4.T[:, :, None] * inv_freq[None, None, :]).reshape(seq // reps, pair)
        half_ff = ff // 2
        vmem = pl.BlockSpec(memory_space=pltpu.VMEM)
        hbm = pl.BlockSpec(memory_space=pl.ANY)
        q, k, v, wo_all, mlp = pl.pallas_call(
            functools.partial(exchange_kernel, 256, head_dim),
            in_specs=[vmem] * 11,
            out_specs=[hbm] * 5,
            out_shape=[
                jax.ShapeDtypeStruct((tp, seq, pair), BF16),
                jax.ShapeDtypeStruct((tp, pair, seq), BF16),
                jax.ShapeDtypeStruct((tp, seq, pair), BF16),
                jax.ShapeDtypeStruct((tp, 2, ctx_cols // 2, width), BF16),
                jax.ShapeDtypeStruct((tokens, width), F32),
            ],
            scratch_shapes=[
                pltpu.VMEM((tp, chunk, width), BF16),
                pltpu.VMEM((tp, groups, slot_cols, width), BF16),
                pltpu.VMEM((tp, 2, width, half_ff), BF16),
                pltpu.VMEM((tp, 2, half_ff, width), BF16),
                pltpu.VMEM((tokens, width), BF16),
                pltpu.VMEM((tokens, width), F32),
                pltpu.VMEM((2, chunk, width), BF16),
                pltpu.VMEM((seq, pair), F32),
                pltpu.VMEM((seq, pair), F32),
                pltpu.VMEM((2, tp, chunk, pair), BF16),
                pltpu.VMEM((2, tp, pair, chunk), BF16),
                pltpu.VMEM((2, tp, chunk, pair), BF16),
                pltpu.SemaphoreType.DMA((4, 15)),
                pltpu.SemaphoreType.DMA((4, 15)),
                pltpu.SemaphoreType.DMA((9,)),
                pltpu.SemaphoreType.DMA((9,)),
                pltpu.SemaphoreType.DMA((2,)),
                pltpu.SemaphoreType.DMA((2, 3)),
            ],
            compiler_params=pltpu.CompilerParams(vmem_limit_bytes=VMEM_LIMIT, collective_id=0, has_side_effects=True),
            cost_estimate=pl.CostEstimate(flops=4 * tokens * width * ff * tp, bytes_accessed=4 * tokens * width * 2, transcendentals=0),
            name='exchange',
        )(x, mlp_gain.reshape(1, width), mlp_bias.reshape(1, width), attn_gain.reshape(1, width), attn_bias.reshape(1, width),
          w_up, w_down.reshape(2, half_ff, width),
          w_qkv.transpose(1, 2, 0), w_out.reshape(2, ctx_cols // 2, width), jnp.cos(angles), jnp.sin(angles))
        wo_all = wo_all.reshape(tp * ctx_cols, width)

        q_rows, kv_cols = 256, 512
        ctx = pl.pallas_call(
            functools.partial(attn_kernel, head_dim, q_rows, kv_cols),
            grid=(tp,),
            in_specs=[
                pl.BlockSpec((1, seq, pair), lambda p: (p, 0, 0)),
                pl.BlockSpec((1, pair, seq), lambda p: (p, 0, 0)),
                pl.BlockSpec((1, seq, pair), lambda p: (p, 0, 0)),
            ],
            out_specs=hbm,
            out_shape=jax.ShapeDtypeStruct((tp, chunk, tp * pair), BF16),
            scratch_shapes=[
                pltpu.VMEM((2, q_rows, seq), F32),
                pltpu.VMEM((2, seq, pair), BF16),
                pltpu.VMEM((tp, 2, chunk, pair), BF16),
                pltpu.SemaphoreType.DMA((tp, 9)),
                pltpu.SemaphoreType.DMA((tp, 9)),
                pltpu.SemaphoreType.DMA((2,)),
            ],
            compiler_params=pltpu.CompilerParams(dimension_semantics=('arbitrary',), vmem_limit_bytes=VMEM_LIMIT, collective_id=1, has_side_effects=True),
            cost_estimate=pl.CostEstimate(flops=8 * seq * seq * pair * tp, bytes_accessed=2 * seq * width * 4, transcendentals=0),
            name='attn',
        )(q, k, v)

        rows = 512
        nt = tokens // rows
        y = pl.pallas_call(
            final_kernel,
            grid=(nt,),
            in_specs=[
                pl.BlockSpec((rows, width), lambda t: (t, 0)),
                pl.BlockSpec((width, width), lambda t: (0, 0)),
                pl.BlockSpec((rows, width), lambda t: (t, 0)),
            ],
            out_specs=pl.BlockSpec((rows, width), lambda t: (t, 0)),
            out_shape=jax.ShapeDtypeStruct((tokens, width), BF16),
            compiler_params=params(('arbitrary',)),
            cost_estimate=pl.CostEstimate(flops=2 * tokens * width * width, bytes_accessed=tokens * width * 10, transcendentals=0),
            name='final',
        )(ctx.reshape(tokens, width), wo_all, mlp)
        return y.reshape(batch, chunk, width)

    return jax.shard_map(local_layer, mesh=mesh, in_specs=(P('dp', 'tp', None), P(), P(), P(), P(), P(None, 'tp', None), P('tp', None), P(None, 'tp'), P('tp', None), P()), out_specs=P('dp', 'tp', None), check_vma=False)
```

```python
import functools

import jax
import jax.numpy as jnp
from jax import lax
from jax.experimental import pallas as pl
from jax.experimental.pallas import tpu as pltpu
from jax.sharding import PartitionSpec as P

BF16 = jnp.bfloat16
F32 = jnp.float32
VMEM_LIMIT = 60 * 1024 * 1024
MESH = pl.DeviceIdType.MESH


OUTWARD, FORWARD = (0, 1), (7, 8)
SEAT = (0, 8, 1, 3, 2, 5, 4, 6, 7)
DIRECT, LANDING = (0, 1, 2, 3, 4, 5, 6), (2, 3, 4, 5, 6, 7, 8)


class Places:
    def __init__(self, tp):
        self.me = lax.axis_index('tp')
        self.core = lax.rem(self.me, 2)
        self.right, self.left, self.far = lax.rem(self.me + 2, tp), lax.rem(self.me + tp - 2, tp), lax.rem(self.me + 4, tp)
        self.sib = self.other(self.me)
        self.left_sib, self.right_sib, self.far_sib = self.other(self.left), self.other(self.right), self.other(self.far)

    def other(self, device):
        return device + 1 - 2 * self.core

    def route(self, kind):
        me, left, right = self.me, self.left, self.right
        return (
            (right, self.far, None, 0),
            (left, self.far_sib, None, 1),
            (self.sib, self.sib, me, None),
            (right, right, me, None),
            (left, left, me, None),
            (self.right_sib, self.right_sib, me, None),
            (self.left_sib, self.left_sib, me, None),
            (right, None, left, None),
            (self.left_sib, None, right, None),
        )[kind]


def norm_rows(rows, gain, bias):
    rows32 = rows.astype(F32)
    mean = jnp.mean(rows32, axis=-1, keepdims=True)
    centered = rows32 - mean
    var = jnp.mean(centered * centered, axis=-1, keepdims=True)
    return (centered * lax.rsqrt(var + 1e-5) * gain + bias).astype(BF16)


def swap_halves(vals, lane_mod, half):
    width = vals.shape[-1]
    return jnp.where(lane_mod < half, pltpu.roll(vals, width - half, 1), pltpu.roll(vals, half, 1))


def attn_kernel(head_dim, rows, chunk, q_ref, k_ref, v_ref, ctx_ref, s_ref, o_ref, relay_ref, send, recv, own_sem):
    p, tp = pl.program_id(0), ctx_ref.shape[0]
    place = Places(tp)
    me = place.me
    seq, pair = o_ref.shape[1:]
    tok = seq // tp
    slot = lax.rem(p, 2)

    def ship(step, kind):
        to, block, origin, relay = place.route(kind)
        if kind in FORWARD:
            src = relay_ref.at[step, FORWARD.index(kind)]
        else:
            src = o_ref.at[lax.rem(step, 2), pl.ds(pl.multiple_of(block * tok, tok), tok), :]
        dst = ctx_ref.at[origin, step] if relay is None else relay_ref.at[step, relay]
        return pltpu.make_async_remote_copy(src_ref=src, dst_ref=dst, send_sem=send.at[step, kind], recv_sem=recv.at[step, kind], device_id={'tp': to}, device_id_type=MESH)

    def keep(step):
        src = o_ref.at[lax.rem(step, 2), pl.ds(pl.multiple_of(me * tok, tok), tok), :]
        return pltpu.make_async_copy(src, ctx_ref.at[me, step], own_sem.at[lax.rem(step, 2)])

    def drain(step):
        for kind in DIRECT:
            ship(step, kind).wait_send()
        keep(step).wait()

    def send_rows(start):
        for kind in DIRECT:
            mine = place.route(kind)[1] * tok // (seq // 2) == start // (seq // 2)
            pl.when(mine)(ship(p, kind).start)

    def pass_on(step):
        for out, kind in zip(OUTWARD, FORWARD):
            ship(step, out).wait_recv()
            ship(step, kind).start()

    @pl.when(p == 0)
    def _():
        barrier = pltpu.get_barrier_semaphore()
        for r in range(1, tp):
            pl.semaphore_signal(barrier, inc=1, device_id={'tp': lax.rem(me + r, tp)}, device_id_type=MESH)
        pl.semaphore_wait(barrier, tp - 1)

    @pl.when(p >= 2)
    def _():
        drain(p - 2)

    units = [(r, h) for r in range(0, seq, rows) for h in range(pair // head_dim)]
    lane = lax.broadcasted_iota(jnp.int32, (rows, pair), 1)

    def fold(op, vals, carry):
        for t in range(0, vals.shape[1], 128):
            part = vals[:, t:t + 128]
            carry = part if carry is None else op(carry, part)
        return carry

    def load_query(unit):
        r, h = unit
        q = q_ref[0, r:r + rows, :]
        return jnp.where(lane // head_dim == h, q, jnp.zeros_like(q))

    def scores(unit, buf, q, cols, m):
        r, (c, size) = unit[0], cols
        s = jnp.dot(q, k_ref[0, :, c:c + size], preferred_element_type=F32)
        if c + size > r:
            row = lax.broadcasted_iota(jnp.int32, s.shape, 0) + r
            col = lax.broadcasted_iota(jnp.int32, s.shape, 1) + c
            s = jnp.where(col <= row, s, -1e30)
        s_ref[buf, :, c:c + size] = s
        return fold(jnp.maximum, s, m)

    def weigh(buf, m, cols, total, acc):
        c, size = cols
        e = jnp.exp(s_ref[buf, :, c:c + size] - m)
        total = fold(jnp.add, e, total)
        pv = jnp.dot(e.astype(BF16), v_ref[0, c:c + size, :], preferred_element_type=F32)
        return total, pv if acc is None else acc + pv

    def starts(unit):
        end = unit[0] + rows
        return [(c, min(chunk, end - c)) for c in range(0, end, chunk)]

    q_next, m_next = load_query(units[0]), None
    for c in starts(units[0]):
        m_next = scores(units[0], 0, q_next, c, m_next)
    for n, unit in enumerate(units):
        m = jnp.max(m_next, axis=1, keepdims=True)
        total = acc = m_next = None
        follow = units[n + 1] if n + 1 < len(units) else None
        todo = starts(follow) if follow else []
        if follow:
            q_next = load_query(follow)
        for j in range(max(len(todo), len(starts(unit)))):
            if j < len(todo):
                m_next = scores(follow, (n + 1) % 2, q_next, todo[j], m_next)
            if j < len(starts(unit)):
                total, acc = weigh(n % 2, m, starts(unit)[j], total, acc)
        r, h = unit
        out = (acc / jnp.sum(total, axis=1, keepdims=True)).astype(BF16)
        o_ref[slot, r:r + rows, h * head_dim:(h + 1) * head_dim] = out[:, h * head_dim:(h + 1) * head_dim]
        if follow and r < seq // 2 <= follow[0]:
            send_rows(0)

    send_rows(seq // 2)
    keep(p).start()

    @pl.when(p >= 1)
    def _():
        pass_on(p - 1)

    @pl.when(p == pl.num_programs(0) - 1)
    def _():
        pass_on(p)
        drain(p - 1)
        drain(p)
        for step in range(recv.shape[0]):
            for kind in FORWARD:
                ship(step, kind).wait_send()
            for kind in LANDING:
                ship(step, kind).wait_recv()


def exchange_kernel(sub, head_dim, x_ref, mgain_ref, mbias_ref, again_ref, abias_ref, up_ref, down_ref, wqkv_ref, wo_ref, cos4_ref, sin4_ref,
                    q_ref, k_ref, v_ref, wo_all, mlp_ref,
                    xs_ref, wqkv_all, up_all, down_all, m_ref, acc_ref, relay_ref, cos_ref, sin_ref, q_st, k_st, v_st,
                    send, recv, xsend, xrecv, own_sem, out_sem):
    tp = xs_ref.shape[0]
    place = Places(tp)
    me, core, sib = place.me, place.core, place.sib
    right, left, far = place.right, place.left, place.far
    dp = lax.axis_index('dp')
    hz = lax.rem(dp, 2)
    twin = dp + 1 - 2 * hz
    tok = x_ref.shape[1]
    pair = q_ref.shape[2]
    tokens, width = acc_ref.shape

    barrier = pltpu.get_barrier_semaphore()
    for r in range(1, tp):
        pl.semaphore_signal(barrier, inc=1, device_id={'tp': lax.rem(me + r, tp)}, device_id_type=MESH)
    pl.semaphore_signal(barrier, inc=1, device_id={'dp': twin}, device_id_type=MESH)
    pl.semaphore_wait(barrier, tp)

    weights = ((up_ref, up_all, True), (down_ref, down_all, True), (wqkv_ref, wqkv_all, False), (wo_ref, wo_all, True))
    UP, DOWN, QKV, OUT = range(4)

    half_ff = up_all.shape[3]

    def up_cols(n):
        start = n * half_ff
        return up_ref.at[:, pl.ds(start if isinstance(n, int) else pl.multiple_of(start, half_ff), half_ff)]

    def whole(ref, shared):
        return ref.at[hz] if shared else ref

    def link(w, k):
        own, every, shared = weights[w]
        rows = every.shape[2]
        mine = up_cols(hz) if w == UP else whole(own, shared)

        def part(s):
            return whole(every.at[s], shared)

        def quarter(s, n):
            if shared:
                return every.at[s, hz, n * (rows // 2):(n + 1) * (rows // 2), :]
            return every.at[s, n]

        if k == 0:
            src, dst, dev = mine, part(me), {'tp': right}
        elif k == 1:
            src, dst, dev = mine, part(me), {'tp': left}
        elif k == 2:
            src, dst, dev = (up_cols(0), every.at[me, 0], {'tp': sib}) if w == UP else (own, every.at[me], {'tp': sib})
        elif k == 14:
            src, dst, dev = up_cols(1), every.at[me, 1], {'tp': sib}
        elif k == 3:
            src, dst, dev = quarter(left, 0), quarter(left, 0), {'tp': right}
        elif k == 4:
            src, dst, dev = quarter(right, 1), quarter(right, 1), {'tp': left}
        elif k < 8:
            s = (left, right, far)[k - 5]
            src, dst, dev = part(s), part(s), {'dp': twin}
        elif k < 11:
            s = (left, right, far)[k - 8]
            src, dst, dev = part(s), part(s), {'tp': sib}
        else:
            s = (left, right, far)[k - 11]
            src, dst, dev = every.at[s, 1 - hz], every.at[s, 1 - hz], {'tp': sib}
        return pltpu.make_async_remote_copy(src_ref=src, dst_ref=dst, send_sem=send.at[w, k], recv_sem=recv.at[w, k], device_id=dev, device_id_type=MESH)

    started = []

    def go(w, *kinds):
        for k in kinds:
            link(w, k).start()
            started.append((w, k))

    def arrived(w, *kinds):
        for k in kinds:
            link(w, k).wait_recv()

    def near(w):
        shared = weights[w][2]
        arrived(w, 0, 1)
        go(w, 3, 4)
        if shared:
            go(w, 5, 6)
        go(w, 8, 9)

    def distant(w):
        shared = weights[w][2]
        arrived(w, 3, 4)
        if shared:
            go(w, 7)
        go(w, 10)

    def token_block(kind):
        to, block, origin, relay = place.route(kind)
        src = relay_ref.at[FORWARD.index(kind)] if kind in FORWARD else x_ref.at[block]
        dst = xs_ref.at[origin] if relay is None else relay_ref.at[relay]
        return pltpu.make_async_remote_copy(src_ref=src, dst_ref=dst, send_sem=xsend.at[kind], recv_sem=xrecv.at[SEAT[kind]], device_id={'tp': to}, device_id_type=MESH)

    def tables(j):
        quarter = cos4_ref.shape[1] // 4
        lane4 = lax.broadcasted_iota(jnp.int32, cos4_ref.shape, 1)
        rows_j = slice(j * cos4_ref.shape[0], (j + 1) * cos4_ref.shape[0])
        sign = jnp.where(lane4 % head_dim < quarter, -1.0, 1.0).astype(F32)
        for src, dst, factor in ((cos4_ref, cos_ref, None), (sin4_ref, sin_ref, sign)):
            vals = jnp.where(lane4 // quarter == j, src[...], 0.0)
            vals = vals + pltpu.roll(vals, quarter, 1)
            vals = vals + pltpu.roll(vals, 2 * quarter, 1)
            dst[rows_j, :] = vals if factor is None else vals * factor

    def outputs(n, s):
        block = lax.rem(n, 2)
        at = pl.ds(pl.multiple_of(s * tok, tok), tok)
        return [
            pltpu.make_async_copy(q_st.at[block], q_ref.at[:, at, :], out_sem.at[block, 0]),
            pltpu.make_async_copy(k_st.at[block], k_ref.at[:, :, at], out_sem.at[block, 1]),
            pltpu.make_async_copy(v_st.at[block], v_ref.at[:, at, :], out_sem.at[block, 2]),
        ]

    sources = (
        lambda n: me + n * (1 - 2 * core),
        lambda n: lax.rem(me + 2 + 4 * (n - 2), tp),
        lambda n: place.other(lax.rem(me + 2 + 4 * (n - 4), tp)),
        lambda n: far + (n - 6) * (1 - 2 * core),
    )

    def project_pair(g):
        lax.fori_loop(2 * g, 2 * g + 2, functools.partial(project, g), 0)

    def project(g, n, carry):
        s, block = sources[g](n), lax.rem(n, 2)
        if g > 0:
            pltpu.make_async_remote_copy(src_ref=x_ref.at[0], dst_ref=xs_ref.at[s], send_sem=xsend.at[0], recv_sem=xrecv.at[n], device_id={'tp': right}, device_id_type=MESH).wait_recv()
            for copy in outputs(n - 2, sources[g - 1](n - 2)):
                copy.wait()
        normed = norm_rows(xs_ref[s], again_ref[...], abias_ref[...])
        at = pl.ds(pl.multiple_of(s * tok, tok), tok)
        cos_tab, sin_tab = cos_ref[at, :], sin_ref[at, :]
        lane = lax.broadcasted_iota(jnp.int32, (tok, pair), 1)
        first = lane < head_dim
        lane_mod = lane % head_dim

        def rotate(vals):
            vals = vals.astype(BF16).astype(F32)
            return (vals * cos_tab + swap_halves(vals, lane_mod, head_dim // 2) * sin_tab).astype(BF16).astype(F32)

        for p in range(tp // 2):
            w = wqkv_all[2 * p:2 * p + 2].reshape(6 * pair, width)
            both = lax.dot_general(normed, w, (((1,), (1,)), ((), ())), preferred_element_type=F32)
            for h in range(2):
                t0, t1, t2 = [both[:, (3 * h + t) * pair:(3 * h + t + 1) * pair] for t in range(3)]
                q_st[block, 2 * p + h] = (rotate(jnp.where(first, t0, t1)) * head_dim ** -0.5).astype(BF16)
                keys = rotate(jnp.where(first, t2, t0)).T.astype(BF16)
                k_st[block, 2 * p + h, :head_dim, :] = keys[head_dim:, :]
                k_st[block, 2 * p + h, head_dim:, :] = keys[:head_dim, :]
                v_st[block, 2 * p + h] = jnp.where(first, t1, t2).astype(BF16)
        for copy in outputs(n, s):
            copy.start()
        return carry

    def gelu(pre):
        return (0.5 * pre * (1.0 + lax.erf(pre * (0.5 ** 0.5)))).astype(BF16)

    def mlp(first, parts):
        ups = [p[0] for p in parts]
        downs = [p[1] for p in parts]

        def body(t, carry):
            base = pl.multiple_of(t * 2 * sub, 2 * sub)

            def expand(h):
                rows_in = m_ref[pl.ds(base + h * sub, sub), :]
                return [jnp.dot(rows_in, u[...], preferred_element_type=F32) for u in ups]

            pre = expand(0)
            for h in range(2):
                following = expand(1) if h == 0 else None
                act = jnp.concatenate([gelu(p) for p in pre], axis=1)
                down_w = jnp.concatenate([d[...] for d in downs], axis=0)
                out = jnp.dot(act, down_w, preferred_element_type=F32)
                rows_out = pl.ds(base + h * sub, sub)
                if first:
                    acc_ref[rows_out, :] = out + x_ref[2 * t + h].astype(F32)
                else:
                    acc_ref[rows_out, :] += out
                pre = following
            return carry

        lax.fori_loop(0, tokens // (2 * sub), body, 0)

    def halves(s, n):
        return up_all.at[s, n], down_all.at[s, n]

    local = pltpu.make_async_copy(wo_ref, wo_all.at[me], own_sem.at[0])
    done = pltpu.make_async_copy(acc_ref, mlp_ref, own_sem.at[1])
    for w in (UP, DOWN, QKV, OUT):
        go(w, 0, 1, 2)
    go(UP, 14)
    local.start()
    token_block(2).start()

    def norm(t, carry):
        m_ref[pl.ds(pl.multiple_of(t * tok, tok), tok), :] = norm_rows(x_ref[t], mgain_ref[...], mbias_ref[...])
        return carry

    lax.fori_loop(0, tp, norm, 0)
    arrived(UP, 2, 14)
    arrived(DOWN, 2)
    near(UP)
    mlp(True, [(up_cols(0), down_ref.at[0]), (up_cols(1), down_ref.at[1]), halves(sib, 0), halves(sib, 1)])
    near(DOWN)
    arrived(UP, 8, 9)
    arrived(DOWN, 8, 9)
    left_sib, right_sib, far_sib = place.left_sib, place.right_sib, place.far_sib
    mlp(False, [halves(left, hz), halves(right, hz), halves(left_sib, hz), halves(right_sib, hz)])
    near(QKV)
    for kind in (0, 1, 3, 4, 5, 6):
        token_block(kind).start()
    for j in range(4):
        tables(j)
    xs_ref[me] = x_ref[me]
    wqkv_all[me] = wqkv_ref[...]
    distant(UP)
    distant(DOWN)
    for w in (UP, DOWN):
        arrived(w, 5, 6)
        go(w, 11, 12)
    arrived(UP, 11, 12)
    arrived(DOWN, 11, 12)
    mlp(False, [halves(left, 1 - hz), halves(right, 1 - hz), halves(left_sib, 1 - hz), halves(right_sib, 1 - hz)])
    near(OUT)
    distant(QKV)
    for out, kind in zip(OUTWARD, FORWARD):
        token_block(out).wait_recv()
        token_block(kind).start()
    arrived(QKV, 2, 8, 9, 10)
    token_block(2).wait_recv()
    project_pair(0)
    distant(OUT)
    project_pair(1)
    for w in (UP, DOWN):
        arrived(w, 7)
        go(w, 13)
    for w in (UP, DOWN):
        arrived(w, 10, 13)
    mlp(False, [halves(far, hz), halves(far, 1 - hz), halves(far_sib, hz), halves(far_sib, 1 - hz)])
    done.start()
    arrived(OUT, 5, 6, 7)
    go(OUT, 11, 12, 13)
    project_pair(2)
    project_pair(3)
    for n in (6, 7):
        for copy in outputs(n, sources[3](n)):
            copy.wait()
    arrived(OUT, 2, 8, 9, 10, 11, 12, 13)
    for w, k in started:
        link(w, k).wait_send()
    for kind in range(9):
        token_block(kind).wait_send()
    local.wait()
    done.wait()


def final_kernel(ctx_ref, wo_ref, rest_ref, y_ref):
    ctx = jnp.concatenate([
        jnp.concatenate([ctx_ref[b, p] for p in range(ctx_ref.shape[1])], axis=1) for b in range(ctx_ref.shape[0])], axis=0)
    attn = jnp.dot(ctx, wo_ref[...], preferred_element_type=F32)
    y_ref[...] = (rest_ref[...] + attn).astype(BF16)


def params(sem):
    return pltpu.CompilerParams(dimension_semantics=sem, vmem_limit_bytes=VMEM_LIMIT)


def solution(mesh):
    tp = mesh.shape['tp']

    def local_layer(x, attn_gain, attn_bias, mlp_gain, mlp_bias, w_qkv, w_out, w_up, w_down, positions):
        batch, chunk, width = x.shape
        per_dev = batch // tp
        groups, slot_cols = w_qkv.shape[1:]
        ctx_cols = w_out.shape[0]
        head_dim = (slot_cols - ctx_cols // groups) // 2
        pair = groups * head_dim
        seq = chunk * tp
        ff = w_up.shape[1]
        tokens = batch * chunk
        half = head_dim // 2

        inv_freq = 10000.0 ** (-2.0 * jnp.arange(half, dtype=F32) / head_dim)
        reps = pair // half
        pos4 = positions.astype(F32).reshape(reps, seq // reps)
        angles = (pos4.T[:, :, None] * inv_freq[None, None, :]).reshape(seq // reps, pair)
        half_ff = ff // 2
        vmem = pl.BlockSpec(memory_space=pltpu.VMEM)
        hbm = pl.BlockSpec(memory_space=pl.ANY)
        q, k, v, wo_all, mlp = pl.pallas_call(
            functools.partial(exchange_kernel, 256, head_dim),
            in_specs=[vmem] * 11,
            out_specs=[hbm] * 5,
            out_shape=[
                jax.ShapeDtypeStruct((tp, seq, pair), BF16),
                jax.ShapeDtypeStruct((tp, pair, seq), BF16),
                jax.ShapeDtypeStruct((tp, seq, pair), BF16),
                jax.ShapeDtypeStruct((tp, 2, ctx_cols // 2, width), BF16),
                jax.ShapeDtypeStruct((tokens, width), F32),
            ],
            scratch_shapes=[
                pltpu.VMEM((tp, chunk, width), BF16),
                pltpu.VMEM((tp, groups, slot_cols, width), BF16),
                pltpu.VMEM((tp, 2, width, half_ff), BF16),
                pltpu.VMEM((tp, 2, half_ff, width), BF16),
                pltpu.VMEM((tokens, width), BF16),
                pltpu.VMEM((tokens, width), F32),
                pltpu.VMEM((2, chunk, width), BF16),
                pltpu.VMEM((seq, pair), F32),
                pltpu.VMEM((seq, pair), F32),
                pltpu.VMEM((2, tp, chunk, pair), BF16),
                pltpu.VMEM((2, tp, pair, chunk), BF16),
                pltpu.VMEM((2, tp, chunk, pair), BF16),
                pltpu.SemaphoreType.DMA((4, 15)),
                pltpu.SemaphoreType.DMA((4, 15)),
                pltpu.SemaphoreType.DMA((9,)),
                pltpu.SemaphoreType.DMA((9,)),
                pltpu.SemaphoreType.DMA((2,)),
                pltpu.SemaphoreType.DMA((2, 3)),
            ],
            compiler_params=pltpu.CompilerParams(vmem_limit_bytes=VMEM_LIMIT, collective_id=0, has_side_effects=True),
            cost_estimate=pl.CostEstimate(flops=4 * tokens * width * ff * tp, bytes_accessed=4 * tokens * width * 2, transcendentals=0),
            name='exchange',
        )(x, mlp_gain.reshape(1, width), mlp_bias.reshape(1, width), attn_gain.reshape(1, width), attn_bias.reshape(1, width),
          w_up, w_down.reshape(2, half_ff, width),
          w_qkv.transpose(1, 2, 0), w_out.reshape(2, ctx_cols // 2, width), jnp.cos(angles), jnp.sin(angles))
        wo_all = wo_all.reshape(tp * ctx_cols, width)

        q_rows, kv_cols = 256, 512
        ctx = pl.pallas_call(
            functools.partial(attn_kernel, head_dim, q_rows, kv_cols),
            grid=(tp,),
            in_specs=[
                pl.BlockSpec((1, seq, pair), lambda p: (p, 0, 0)),
                pl.BlockSpec((1, pair, seq), lambda p: (p, 0, 0)),
                pl.BlockSpec((1, seq, pair), lambda p: (p, 0, 0)),
            ],
            out_specs=hbm,
            out_shape=jax.ShapeDtypeStruct((tp, tp, chunk, pair), BF16),
            scratch_shapes=[
                pltpu.VMEM((2, q_rows, seq), F32),
                pltpu.VMEM((2, seq, pair), BF16),
                pltpu.VMEM((tp, 2, chunk, pair), BF16),
                pltpu.SemaphoreType.DMA((tp, 9)),
                pltpu.SemaphoreType.DMA((tp, 9)),
                pltpu.SemaphoreType.DMA((2,)),
            ],
            compiler_params=pltpu.CompilerParams(dimension_semantics=('arbitrary',), vmem_limit_bytes=VMEM_LIMIT, collective_id=1, has_side_effects=True),
            cost_estimate=pl.CostEstimate(flops=8 * seq * seq * pair * tp, bytes_accessed=2 * seq * width * 4, transcendentals=0),
            name='attn',
        )(q, k, v)

        rows = 512
        nt = tokens // rows
        y = pl.pallas_call(
            final_kernel,
            grid=(nt,),
            in_specs=[
                pl.BlockSpec((rows // chunk, tp, chunk, pair), lambda t: (t, 0, 0, 0)),
                pl.BlockSpec((width, width), lambda t: (0, 0)),
                pl.BlockSpec((rows, width), lambda t: (t, 0)),
            ],
            out_specs=pl.BlockSpec((rows, width), lambda t: (t, 0)),
            out_shape=jax.ShapeDtypeStruct((tokens, width), BF16),
            compiler_params=params(('arbitrary',)),
            cost_estimate=pl.CostEstimate(flops=2 * tokens * width * width, bytes_accessed=tokens * width * 10, transcendentals=0),
            name='final',
        )(ctx, wo_all, mlp)
        return y.reshape(batch, chunk, width)

    return jax.shard_map(local_layer, mesh=mesh, in_specs=(P('dp', 'tp', None), P(), P(), P(), P(), P(None, 'tp', None), P('tp', None), P(None, 'tp'), P('tp', None), P()), out_specs=P('dp', 'tp', None), check_vma=False)
```

```python
import functools

import jax
import jax.numpy as jnp
from jax import lax
from jax.experimental import pallas as pl
from jax.experimental.pallas import tpu as pltpu
from jax.sharding import PartitionSpec as P

BF16 = jnp.bfloat16
F32 = jnp.float32
VMEM_LIMIT = 60 * 1024 * 1024
MESH = pl.DeviceIdType.MESH


OUTWARD, FORWARD = (0, 1), (7, 8)
SEAT = (0, 8, 1, 3, 2, 5, 4, 6, 7)
DIRECT, LANDING = (0, 1, 2, 3, 4, 5, 6), (2, 3, 4, 5, 6, 7, 8)


class Places:
    def __init__(self, tp):
        self.me = lax.axis_index('tp')
        self.core = lax.rem(self.me, 2)
        self.right, self.left, self.far = lax.rem(self.me + 2, tp), lax.rem(self.me + tp - 2, tp), lax.rem(self.me + 4, tp)
        self.sib = self.other(self.me)
        self.left_sib, self.right_sib, self.far_sib = self.other(self.left), self.other(self.right), self.other(self.far)

    def other(self, device):
        return device + 1 - 2 * self.core

    def route(self, kind):
        me, left, right = self.me, self.left, self.right
        return (
            (right, self.far, None, 0),
            (left, self.far_sib, None, 1),
            (self.sib, self.sib, me, None),
            (right, right, me, None),
            (left, left, me, None),
            (self.right_sib, self.right_sib, me, None),
            (self.left_sib, self.left_sib, me, None),
            (right, None, left, None),
            (self.left_sib, None, right, None),
        )[kind]


def norm_rows(rows, gain, bias):
    rows32 = rows.astype(F32)
    mean = jnp.mean(rows32, axis=-1, keepdims=True)
    centered = rows32 - mean
    var = jnp.mean(centered * centered, axis=-1, keepdims=True)
    return (centered * lax.rsqrt(var + 1e-5) * gain + bias).astype(BF16)


def swap_halves(vals, lane_mod, half):
    width = vals.shape[-1]
    return jnp.where(lane_mod < half, pltpu.roll(vals, width - half, 1), pltpu.roll(vals, half, 1))


def attn_kernel(head_dim, rows, chunk, q_ref, k_ref, v_ref, ctx_ref, s_ref, o_ref, relay_ref, send, recv, own_sem):
    p, tp = pl.program_id(0), ctx_ref.shape[0]
    place = Places(tp)
    me = place.me
    seq, pair = o_ref.shape[1:]
    tok = seq // tp
    slot = lax.rem(p, 2)

    def ship(step, kind):
        to, block, origin, relay = place.route(kind)
        if kind in FORWARD:
            src = relay_ref.at[step, FORWARD.index(kind)]
        else:
            src = o_ref.at[lax.rem(step, 2), pl.ds(pl.multiple_of(block * tok, tok), tok), :]
        dst = ctx_ref.at[origin, step] if relay is None else relay_ref.at[step, relay]
        return pltpu.make_async_remote_copy(src_ref=src, dst_ref=dst, send_sem=send.at[step, kind], recv_sem=recv.at[step, kind], device_id={'tp': to}, device_id_type=MESH)

    def keep(step):
        src = o_ref.at[lax.rem(step, 2), pl.ds(pl.multiple_of(me * tok, tok), tok), :]
        return pltpu.make_async_copy(src, ctx_ref.at[me, step], own_sem.at[lax.rem(step, 2)])

    def drain(step):
        for kind in DIRECT:
            ship(step, kind).wait_send()
        keep(step).wait()

    def send_rows(start):
        for kind in DIRECT:
            mine = place.route(kind)[1] * tok // (seq // 2) == start // (seq // 2)
            pl.when(mine)(ship(p, kind).start)

    def pass_on(step):
        for out, kind in zip(OUTWARD, FORWARD):
            ship(step, out).wait_recv()
            ship(step, kind).start()

    @pl.when(p == 0)
    def _():
        barrier = pltpu.get_barrier_semaphore()
        for r in range(1, tp):
            pl.semaphore_signal(barrier, inc=1, device_id={'tp': lax.rem(me + r, tp)}, device_id_type=MESH)
        pl.semaphore_wait(barrier, tp - 1)

    @pl.when(p >= 2)
    def _():
        drain(p - 2)

    units = [(r, h) for r in range(0, seq, rows) for h in range(pair // head_dim)]
    lane = lax.broadcasted_iota(jnp.int32, (rows, pair), 1)

    def fold(op, vals, carry):
        for t in range(0, vals.shape[1], 128):
            part = vals[:, t:t + 128]
            carry = part if carry is None else op(carry, part)
        return carry

    def load_query(unit):
        r, h = unit
        q = q_ref[0, r:r + rows, :]
        return jnp.where(lane // head_dim == h, q, jnp.zeros_like(q))

    def scores(unit, buf, q, cols, m):
        r, (c, size) = unit[0], cols
        s = jnp.dot(q, k_ref[0, :, c:c + size], preferred_element_type=F32)
        if c + size > r:
            row = lax.broadcasted_iota(jnp.int32, s.shape, 0) + r
            col = lax.broadcasted_iota(jnp.int32, s.shape, 1) + c
            s = jnp.where(col <= row, s, -1e30)
        s_ref[buf, :, c:c + size] = s
        return fold(jnp.maximum, s, m)

    def weigh(buf, m, cols, total, acc):
        c, size = cols
        e = jnp.exp(s_ref[buf, :, c:c + size] - m)
        total = fold(jnp.add, e, total)
        pv = jnp.dot(e.astype(BF16), v_ref[0, c:c + size, :], preferred_element_type=F32)
        return total, pv if acc is None else acc + pv

    def starts(unit):
        end = unit[0] + rows
        return [(c, min(chunk, end - c)) for c in range(0, end, chunk)]

    q_next, m_next = load_query(units[0]), None
    for c in starts(units[0]):
        m_next = scores(units[0], 0, q_next, c, m_next)
    for n, unit in enumerate(units):
        m = jnp.max(m_next, axis=1, keepdims=True)
        total = acc = m_next = None
        follow = units[n + 1] if n + 1 < len(units) else None
        todo = starts(follow) if follow else []
        if follow:
            q_next = load_query(follow)
        for j in range(max(len(todo), len(starts(unit)))):
            if j < len(todo):
                m_next = scores(follow, (n + 1) % 2, q_next, todo[j], m_next)
            if j < len(starts(unit)):
                total, acc = weigh(n % 2, m, starts(unit)[j], total, acc)
        r, h = unit
        out = (acc / jnp.sum(total, axis=1, keepdims=True)).astype(BF16)
        o_ref[slot, r:r + rows, h * head_dim:(h + 1) * head_dim] = out[:, h * head_dim:(h + 1) * head_dim]
        if follow and r < seq // 2 <= follow[0]:
            send_rows(0)

    send_rows(seq // 2)
    keep(p).start()

    @pl.when(p >= 1)
    def _():
        pass_on(p - 1)

    @pl.when(p == pl.num_programs(0) - 1)
    def _():
        pass_on(p)
        drain(p - 1)
        drain(p)
        for step in range(recv.shape[0]):
            for kind in FORWARD:
                ship(step, kind).wait_send()
            for kind in LANDING:
                ship(step, kind).wait_recv()


def exchange_kernel(sub, head_dim, x_ref, mgain_ref, mbias_ref, again_ref, abias_ref, up_ref, down_ref, wqkv_ref, wo_ref, cos4_ref, sin4_ref,
                    q_ref, k_ref, v_ref, wo_all, mlp_ref,
                    xs_ref, wqkv_all, up_all, down_all, m_ref, acc_ref, relay_ref, cos_ref, sin_ref, q_st, k_st, v_st,
                    send, recv, xsend, xrecv, own_sem, out_sem):
    tp = xs_ref.shape[0]
    place = Places(tp)
    me, core, sib = place.me, place.core, place.sib
    right, left, far = place.right, place.left, place.far
    dp = lax.axis_index('dp')
    hz = lax.rem(dp, 2)
    twin = dp + 1 - 2 * hz
    tok = x_ref.shape[1]
    pair = q_ref.shape[2]
    tokens, width = acc_ref.shape

    barrier = pltpu.get_barrier_semaphore()
    for r in range(1, tp):
        pl.semaphore_signal(barrier, inc=1, device_id={'tp': lax.rem(me + r, tp)}, device_id_type=MESH)
    pl.semaphore_signal(barrier, inc=1, device_id={'dp': twin}, device_id_type=MESH)
    pl.semaphore_wait(barrier, tp)

    weights = ((up_ref, up_all, True), (down_ref, down_all, True), (wqkv_ref, wqkv_all, False), (wo_ref, wo_all, True))
    UP, DOWN, QKV, OUT = range(4)

    half_ff = up_all.shape[3]

    def up_cols(n):
        start = n * half_ff
        return up_ref.at[:, pl.ds(start if isinstance(n, int) else pl.multiple_of(start, half_ff), half_ff)]

    def whole(ref, shared):
        return ref.at[hz] if shared else ref

    def link(w, k):
        own, every, shared = weights[w]
        rows = every.shape[2]
        mine = up_cols(hz) if w == UP else whole(own, shared)

        def part(s):
            return whole(every.at[s], shared)

        def quarter(s, n):
            if shared:
                return every.at[s, hz, n * (rows // 2):(n + 1) * (rows // 2), :]
            return every.at[s, n]

        if k == 0:
            src, dst, dev = mine, part(me), {'tp': right}
        elif k == 1:
            src, dst, dev = mine, part(me), {'tp': left}
        elif k == 2:
            src, dst, dev = (up_cols(0), every.at[me, 0], {'tp': sib}) if w == UP else (own, every.at[me], {'tp': sib})
        elif k == 14:
            src, dst, dev = up_cols(1), every.at[me, 1], {'tp': sib}
        elif k == 3:
            src, dst, dev = quarter(left, 0), quarter(left, 0), {'tp': right}
        elif k == 4:
            src, dst, dev = quarter(right, 1), quarter(right, 1), {'tp': left}
        elif k < 8:
            s = (left, right, far)[k - 5]
            src, dst, dev = part(s), part(s), {'dp': twin}
        elif k < 11:
            s = (left, right, far)[k - 8]
            src, dst, dev = part(s), part(s), {'tp': sib}
        else:
            s = (left, right, far)[k - 11]
            src, dst, dev = every.at[s, 1 - hz], every.at[s, 1 - hz], {'tp': sib}
        return pltpu.make_async_remote_copy(src_ref=src, dst_ref=dst, send_sem=send.at[w, k], recv_sem=recv.at[w, k], device_id=dev, device_id_type=MESH)

    started = []

    def go(w, *kinds):
        for k in kinds:
            link(w, k).start()
            started.append((w, k))

    def arrived(w, *kinds):
        for k in kinds:
            link(w, k).wait_recv()

    def near(w):
        shared = weights[w][2]
        arrived(w, 0, 1)
        go(w, 3, 4)
        if shared:
            go(w, 5, 6)
        go(w, 8, 9)

    def distant(w):
        shared = weights[w][2]
        arrived(w, 3, 4)
        if shared:
            go(w, 7)
        go(w, 10)

    def token_block(kind):
        to, block, origin, relay = place.route(kind)
        src = relay_ref.at[FORWARD.index(kind)] if kind in FORWARD else x_ref.at[block]
        dst = xs_ref.at[origin] if relay is None else relay_ref.at[relay]
        return pltpu.make_async_remote_copy(src_ref=src, dst_ref=dst, send_sem=xsend.at[kind], recv_sem=xrecv.at[SEAT[kind]], device_id={'tp': to}, device_id_type=MESH)

    def tables(j):
        quarter = cos4_ref.shape[1] // 4
        lane4 = lax.broadcasted_iota(jnp.int32, cos4_ref.shape, 1)
        rows_j = slice(j * cos4_ref.shape[0], (j + 1) * cos4_ref.shape[0])
        sign = jnp.where(lane4 % head_dim < quarter, -1.0, 1.0).astype(F32)
        for src, dst, factor in ((cos4_ref, cos_ref, None), (sin4_ref, sin_ref, sign)):
            vals = jnp.where(lane4 // quarter == j, src[...], 0.0)
            vals = vals + pltpu.roll(vals, quarter, 1)
            vals = vals + pltpu.roll(vals, 2 * quarter, 1)
            dst[rows_j, :] = vals if factor is None else vals * factor

    def outputs(n, s):
        block = lax.rem(n, 2)
        at = pl.ds(pl.multiple_of(s * tok, tok), tok)
        return [
            pltpu.make_async_copy(q_st.at[block], q_ref.at[:, at, :], out_sem.at[block, 0]),
            pltpu.make_async_copy(k_st.at[block], k_ref.at[:, :, at], out_sem.at[block, 1]),
            pltpu.make_async_copy(v_st.at[block], v_ref.at[:, at, :], out_sem.at[block, 2]),
        ]

    sources = (
        lambda n: me + n * (1 - 2 * core),
        lambda n: lax.rem(me + 2 + 4 * (n - 2), tp),
        lambda n: place.other(lax.rem(me + 2 + 4 * (n - 4), tp)),
        lambda n: far + (n - 6) * (1 - 2 * core),
    )

    def project_pair(g):
        lax.fori_loop(2 * g, 2 * g + 2, functools.partial(project, g), 0)

    def project(g, n, carry):
        s, block = sources[g](n), lax.rem(n, 2)
        if g > 0:
            pltpu.make_async_remote_copy(src_ref=x_ref.at[0], dst_ref=xs_ref.at[s], send_sem=xsend.at[0], recv_sem=xrecv.at[n], device_id={'tp': right}, device_id_type=MESH).wait_recv()
            for copy in outputs(n - 2, sources[g - 1](n - 2)):
                copy.wait()
        normed = norm_rows(xs_ref[s], again_ref[...], abias_ref[...])
        at = pl.ds(pl.multiple_of(s * tok, tok), tok)
        cos_tab, sin_tab = cos_ref[at, :], sin_ref[at, :]
        lane = lax.broadcasted_iota(jnp.int32, (tok, pair), 1)
        first = lane < head_dim
        lane_mod = lane % head_dim

        def rotate(vals):
            vals = vals.astype(BF16).astype(F32)
            return (vals * cos_tab + swap_halves(vals, lane_mod, head_dim // 2) * sin_tab).astype(BF16).astype(F32)

        for p in range(tp // 2):
            w = wqkv_all[2 * p:2 * p + 2].reshape(6 * pair, width)
            both = lax.dot_general(normed, w, (((1,), (1,)), ((), ())), preferred_element_type=F32)
            for h in range(2):
                t0, t1, t2 = [both[:, (3 * h + t) * pair:(3 * h + t + 1) * pair] for t in range(3)]
                q_st[block, 2 * p + h] = (rotate(jnp.where(first, t0, t1)) * head_dim ** -0.5).astype(BF16)
                keys = rotate(jnp.where(first, t2, t0)).T.astype(BF16)
                k_st[block, 2 * p + h, :head_dim, :] = keys[head_dim:, :]
                k_st[block, 2 * p + h, head_dim:, :] = keys[:head_dim, :]
                v_st[block, 2 * p + h] = jnp.where(first, t1, t2).astype(BF16)
        for copy in outputs(n, s):
            copy.start()
        return carry

    def gelu(pre):
        return (0.5 * pre * (1.0 + lax.erf(pre * (0.5 ** 0.5)))).astype(BF16)

    def mlp(first, parts):
        ups = [p[0] for p in parts]
        downs = [p[1] for p in parts]

        def body(t, carry):
            base = pl.multiple_of(t * 2 * sub, 2 * sub)

            def expand(h):
                rows_in = m_ref[pl.ds(base + h * sub, sub), :]
                return [jnp.dot(rows_in, u[...], preferred_element_type=F32) for u in ups]

            pre = expand(0)
            for h in range(2):
                following = expand(1) if h == 0 else None
                act = jnp.concatenate([gelu(p) for p in pre], axis=1)
                down_w = jnp.concatenate([d[...] for d in downs], axis=0)
                out = jnp.dot(act, down_w, preferred_element_type=F32)
                rows_out = pl.ds(base + h * sub, sub)
                if first:
                    acc_ref[rows_out, :] = out + x_ref[2 * t + h].astype(F32)
                else:
                    acc_ref[rows_out, :] += out
                pre = following
            return carry

        lax.fori_loop(0, tokens // (2 * sub), body, 0)

    def halves(s, n):
        return up_all.at[s, n], down_all.at[s, n]

    local = pltpu.make_async_copy(wo_ref, wo_all.at[me], own_sem.at[0])
    done = pltpu.make_async_copy(acc_ref, mlp_ref, own_sem.at[1])
    for w in (UP, DOWN, QKV, OUT):
        go(w, 0, 1, 2)
    go(UP, 14)
    local.start()
    token_block(2).start()

    def norm(t, carry):
        m_ref[pl.ds(pl.multiple_of(t * tok, tok), tok), :] = norm_rows(x_ref[t], mgain_ref[...], mbias_ref[...])
        return carry

    lax.fori_loop(0, tp, norm, 0)
    arrived(UP, 2, 14)
    arrived(DOWN, 2)
    near(UP)
    mlp(True, [(up_cols(0), down_ref.at[0]), (up_cols(1), down_ref.at[1]), halves(sib, 0), halves(sib, 1)])
    near(DOWN)
    arrived(UP, 8, 9)
    arrived(DOWN, 8, 9)
    left_sib, right_sib, far_sib = place.left_sib, place.right_sib, place.far_sib
    mlp(False, [halves(left, hz), halves(right, hz), halves(left_sib, hz), halves(right_sib, hz)])
    near(QKV)
    for kind in (0, 1, 3, 4, 5, 6):
        token_block(kind).start()
    for j in range(4):
        tables(j)
    xs_ref[me] = x_ref[me]
    wqkv_all[me] = wqkv_ref[...]
    distant(UP)
    distant(DOWN)
    for w in (UP, DOWN):
        arrived(w, 5, 6)
        go(w, 11, 12)
    arrived(UP, 11, 12)
    arrived(DOWN, 11, 12)
    mlp(False, [halves(left, 1 - hz), halves(right, 1 - hz), halves(left_sib, 1 - hz), halves(right_sib, 1 - hz)])
    near(OUT)
    distant(QKV)
    for out, kind in zip(OUTWARD, FORWARD):
        token_block(out).wait_recv()
        token_block(kind).start()
    arrived(QKV, 2, 8, 9, 10)
    token_block(2).wait_recv()
    project_pair(0)
    distant(OUT)
    for w in (UP, DOWN):
        arrived(w, 7)
        go(w, 13)
    for w in (UP, DOWN):
        arrived(w, 10, 13)
    mlp(False, [halves(far, hz), halves(far, 1 - hz), halves(far_sib, hz), halves(far_sib, 1 - hz)])
    done.start()
    arrived(OUT, 5, 6, 7)
    go(OUT, 11, 12, 13)
    project_pair(1)
    project_pair(2)
    project_pair(3)
    for n in (6, 7):
        for copy in outputs(n, sources[3](n)):
            copy.wait()
    arrived(OUT, 2, 8, 9, 10, 11, 12, 13)
    for w, k in started:
        link(w, k).wait_send()
    for kind in range(9):
        token_block(kind).wait_send()
    local.wait()
    done.wait()


def final_kernel(ctx_ref, wo_ref, rest_ref, y_ref):
    ctx = jnp.concatenate([
        jnp.concatenate([ctx_ref[b, p] for p in range(ctx_ref.shape[1])], axis=1) for b in range(ctx_ref.shape[0])], axis=0)
    attn = jnp.dot(ctx, wo_ref[...], preferred_element_type=F32)
    y_ref[...] = (rest_ref[...] + attn).astype(BF16)


def params(sem):
    return pltpu.CompilerParams(dimension_semantics=sem, vmem_limit_bytes=VMEM_LIMIT)


def solution(mesh):
    tp = mesh.shape['tp']

    def local_layer(x, attn_gain, attn_bias, mlp_gain, mlp_bias, w_qkv, w_out, w_up, w_down, positions):
        batch, chunk, width = x.shape
        per_dev = batch // tp
        groups, slot_cols = w_qkv.shape[1:]
        ctx_cols = w_out.shape[0]
        head_dim = (slot_cols - ctx_cols // groups) // 2
        pair = groups * head_dim
        seq = chunk * tp
        ff = w_up.shape[1]
        tokens = batch * chunk
        half = head_dim // 2

        inv_freq = 10000.0 ** (-2.0 * jnp.arange(half, dtype=F32) / head_dim)
        reps = pair // half
        pos4 = positions.astype(F32).reshape(reps, seq // reps)
        angles = (pos4.T[:, :, None] * inv_freq[None, None, :]).reshape(seq // reps, pair)
        half_ff = ff // 2
        vmem = pl.BlockSpec(memory_space=pltpu.VMEM)
        hbm = pl.BlockSpec(memory_space=pl.ANY)
        q, k, v, wo_all, mlp = pl.pallas_call(
            functools.partial(exchange_kernel, 256, head_dim),
            in_specs=[vmem] * 11,
            out_specs=[hbm] * 5,
            out_shape=[
                jax.ShapeDtypeStruct((tp, seq, pair), BF16),
                jax.ShapeDtypeStruct((tp, pair, seq), BF16),
                jax.ShapeDtypeStruct((tp, seq, pair), BF16),
                jax.ShapeDtypeStruct((tp, 2, ctx_cols // 2, width), BF16),
                jax.ShapeDtypeStruct((tokens, width), F32),
            ],
            scratch_shapes=[
                pltpu.VMEM((tp, chunk, width), BF16),
                pltpu.VMEM((tp, groups, slot_cols, width), BF16),
                pltpu.VMEM((tp, 2, width, half_ff), BF16),
                pltpu.VMEM((tp, 2, half_ff, width), BF16),
                pltpu.VMEM((tokens, width), BF16),
                pltpu.VMEM((tokens, width), F32),
                pltpu.VMEM((2, chunk, width), BF16),
                pltpu.VMEM((seq, pair), F32),
                pltpu.VMEM((seq, pair), F32),
                pltpu.VMEM((2, tp, chunk, pair), BF16),
                pltpu.VMEM((2, tp, pair, chunk), BF16),
                pltpu.VMEM((2, tp, chunk, pair), BF16),
                pltpu.SemaphoreType.DMA((4, 15)),
                pltpu.SemaphoreType.DMA((4, 15)),
                pltpu.SemaphoreType.DMA((9,)),
                pltpu.SemaphoreType.DMA((9,)),
                pltpu.SemaphoreType.DMA((2,)),
                pltpu.SemaphoreType.DMA((2, 3)),
            ],
            compiler_params=pltpu.CompilerParams(vmem_limit_bytes=VMEM_LIMIT, collective_id=0, has_side_effects=True),
            cost_estimate=pl.CostEstimate(flops=4 * tokens * width * ff * tp, bytes_accessed=4 * tokens * width * 2, transcendentals=0),
            name='exchange',
        )(x, mlp_gain.reshape(1, width), mlp_bias.reshape(1, width), attn_gain.reshape(1, width), attn_bias.reshape(1, width),
          w_up, w_down.reshape(2, half_ff, width),
          w_qkv.transpose(1, 2, 0), w_out.reshape(2, ctx_cols // 2, width), jnp.cos(angles), jnp.sin(angles))
        wo_all = wo_all.reshape(tp * ctx_cols, width)

        q_rows, kv_cols = 256, 512
        ctx = pl.pallas_call(
            functools.partial(attn_kernel, head_dim, q_rows, kv_cols),
            grid=(tp,),
            in_specs=[
                pl.BlockSpec((1, seq, pair), lambda p: (p, 0, 0)),
                pl.BlockSpec((1, pair, seq), lambda p: (p, 0, 0)),
                pl.BlockSpec((1, seq, pair), lambda p: (p, 0, 0)),
            ],
            out_specs=hbm,
            out_shape=jax.ShapeDtypeStruct((tp, tp, chunk, pair), BF16),
            scratch_shapes=[
                pltpu.VMEM((2, q_rows, seq), F32),
                pltpu.VMEM((2, seq, pair), BF16),
                pltpu.VMEM((tp, 2, chunk, pair), BF16),
                pltpu.SemaphoreType.DMA((tp, 9)),
                pltpu.SemaphoreType.DMA((tp, 9)),
                pltpu.SemaphoreType.DMA((2,)),
            ],
            compiler_params=pltpu.CompilerParams(dimension_semantics=('arbitrary',), vmem_limit_bytes=VMEM_LIMIT, collective_id=1, has_side_effects=True),
            cost_estimate=pl.CostEstimate(flops=8 * seq * seq * pair * tp, bytes_accessed=2 * seq * width * 4, transcendentals=0),
            name='attn',
        )(q, k, v)

        rows = 512
        nt = tokens // rows
        y = pl.pallas_call(
            final_kernel,
            grid=(nt,),
            in_specs=[
                pl.BlockSpec((rows // chunk, tp, chunk, pair), lambda t: (t, 0, 0, 0)),
                pl.BlockSpec((width, width), lambda t: (0, 0)),
                pl.BlockSpec((rows, width), lambda t: (t, 0)),
            ],
            out_specs=pl.BlockSpec((rows, width), lambda t: (t, 0)),
            out_shape=jax.ShapeDtypeStruct((tokens, width), BF16),
            compiler_params=params(('arbitrary',)),
            cost_estimate=pl.CostEstimate(flops=2 * tokens * width * width, bytes_accessed=tokens * width * 10, transcendentals=0),
            name='final',
        )(ctx, wo_all, mlp)
        return y.reshape(batch, chunk, width)

    return jax.shard_map(local_layer, mesh=mesh, in_specs=(P('dp', 'tp', None), P(), P(), P(), P(), P(None, 'tp', None), P('tp', None), P(None, 'tp'), P('tp', None), P()), out_specs=P('dp', 'tp', None), check_vma=False)
```
